16 devices in a mesh: dp: 1, sp: 16 (over x, y, z, core).
Axes of the slice: x: 2, y: 2, z: 2, core: 2. Of those that a mesh axis runs over, the one named last changes fastest.
Arguments:
- x: bfloat16 [8192, 2560], P(('dp', 'sp'))
- gain: bfloat16 [2560], replicated
- wq: bfloat16 [2560, 2048], P('sp')
- wk: bfloat16 [2560, 1024], P('sp')
- wv: bfloat16 [2560, 1024], P('sp')
- wo: bfloat16 [2048, 2560], P('sp')
Outputs:
- output: bfloat16 [8192, 2560], P(('dp', 'sp'))
All inputs are finite; a program needn't handle non-finite values.
Results may differ from the reference program's by a relative error of at most 0.012.
Values are sent between devices in bfloat16 or wider.
A program may use at most 2 GiB of HBM per device.

```python
import jax
import jax.numpy as jnp
from jax import lax

ROWS = 8192
D = 2560
HEADS = 8
KV_HEADS = 4
HEAD = 256
THETA = 10000


def setup_inputs(seed: int = 0, part: int = 0) -> dict:
    kx, kn, kq, kk, kv, ko = jax.random.split(jax.random.key(seed), 6)

    def weights(key, rows, columns):
        return jax.random.normal(key, (rows, columns), jnp.float32) * rows**-0.5

    drawn = {
        "x": jax.random.normal(jax.random.fold_in(kx, part), (ROWS, D), jnp.float32),
        "gain": 1 + 0.1 * jax.random.normal(kn, (D,), jnp.float32),
        "wq": 2 * weights(kq, D, HEADS * HEAD),
        "wk": 2 * weights(kk, D, KV_HEADS * HEAD),
        "wv": 4 * weights(kv, D, KV_HEADS * HEAD),
        "wo": weights(ko, HEADS * HEAD, D),
    }
    return {k: v.astype(jnp.bfloat16) for k, v in drawn.items()}


def normed(x, gain):
    wide = x.astype(jnp.float32)
    scale = lax.rsqrt(jnp.mean(wide * wide, -1, keepdims=True) + 1e-6)
    return (wide * scale * gain.astype(jnp.float32)).astype(jnp.bfloat16)


def turned(t, place, theta):
    half = t.shape[-1] // 2
    angle = place.astype(jnp.float32)[:, None] * theta ** (-jnp.arange(half, dtype=jnp.float32) / half)
    cos, sin = jnp.cos(angle)[:, None], jnp.sin(angle)[:, None]
    a, b = t[..., :half].astype(jnp.float32), t[..., half:].astype(jnp.float32)
    return jnp.concatenate([a * cos - b * sin, b * cos + a * sin], -1).astype(jnp.bfloat16)


def matmul(a, w):
    return jnp.dot(a, w, preferred_element_type=jnp.float32).astype(jnp.bfloat16)


def einsum(form, a, b):
    return jnp.einsum(form, a.astype(jnp.float32), b.astype(jnp.float32))


def attention(q, k, v):
    scores = einsum("tgsd,ugd->gstu", q, k) * q.shape[-1] ** -0.5
    token = jnp.arange(q.shape[0])
    scores = jnp.where(token[:, None] >= token, scores, -jnp.inf)
    weights = jax.nn.softmax(scores, -1).astype(jnp.bfloat16)
    return einsum("gstu,ugd->tgsd", weights, v).astype(jnp.bfloat16)


def reference(x, gain, wq, wk, wv, wo):
    a, place = normed(x, gain), jnp.arange(ROWS)
    q = turned(matmul(a, wq).reshape(ROWS, HEADS, HEAD), place, THETA).reshape(ROWS, KV_HEADS, -1, HEAD)
    k = turned(matmul(a, wk).reshape(ROWS, KV_HEADS, HEAD), place, THETA)
    v = matmul(a, wv).reshape(ROWS, KV_HEADS, HEAD)
    seen = attention(q, k, v).reshape(ROWS, HEADS * HEAD)
    return (x.astype(jnp.float32) + jnp.dot(seen, wo, preferred_element_type=jnp.float32)).astype(jnp.bfloat16)
```

```python
import functools

import jax
import jax.numpy as jnp
from jax import lax
from jax.experimental import pallas as pl
from jax.experimental.pallas import tpu as pltpu
from jax.sharding import PartitionSpec as P

HEAD = 256
THETA = 10000
D = 2560
OWN = 512
TOK = 1024
CHIPS = 8
NEG = -1e30
HIDDEN = 2 * NEG
LOG2E = 1.4426950408889634
VMEM = 62 * 2**20
MESH = pl.DeviceIdType.MESH
X, Y, Z = 4, 2, 1
ORDERS = ((X, Y, Z), (Y, Z, X), (Z, X, Y))
SENDS = ((0, ()), (1, ()), (1, (0,)), (2, ()), (2, (0,)), (2, (1,)), (2, (0, 1)))
HBM = pltpu.HBM


def flip(v, *bits):
    out = v
    for w in bits:
        out = out + w * (1 - 2 * lax.rem(lax.div(v, w), 2))
    return out


def bits_of(mask):
    return [w for w in (1, 2, 4, 8) if mask & w]


def remote(src, dst, send, recv, device):
    return pltpu.make_async_remote_copy(src_ref=src, dst_ref=dst, send_sem=send, recv_sem=recv, device_id={"sp": device}, device_id_type=MESH)


def meet(me):
    barrier = pltpu.get_barrier_semaphore()
    for mask in range(1, 16):
        pl.semaphore_signal(barrier, inc=1, device_id={"sp": flip(me, *bits_of(mask))}, device_id_type=MESH)
    pl.semaphore_wait(barrier, 15)


def dot(a, b, ca, cb):
    return lax.dot_general(a, b, (((ca,), (cb,)), ((), ())), preferred_element_type=jnp.float32)


class Gather:
    def __init__(self, at, thirds, me, send_sem, recv_sem):
        self.at, self.thirds, self.me, self.chip, self.send_sem, self.recv_sem = at, thirds, me, lax.div(me, 2), send_sem, recv_sem

    def copy(self, i, s):
        order = ORDERS[i]
        link, path = SENDS[s]
        first, rows = self.thirds[i]
        view = self.at(flip(self.chip, *[order[n] for n in path]), first, rows)
        return remote(view, view, self.send_sem.at[7 * i + s], self.recv_sem.at[7 * i + s], flip(self.me, 2 * order[link]))

    def start(self, *sends):
        for s in sends:
            for i in range(3):
                self.copy(i, s).start()

    def arrived(self, *sends):
        for s in sends:
            for i in range(3):
                self.copy(i, s).wait_recv()

    def landed(self, i, s):
        order = ORDERS[i]
        link, path = SENDS[s]
        first, rows = self.thirds[i]
        return self.at(flip(self.chip, order[link], *[order[n] for n in path]), first, rows)

    def sent(self):
        for i in range(3):
            for s in range(7):
                self.copy(i, s).wait_send()


def _project(x_ref, gain_ref, cos_ref, sin_ref, wq_ref, wk_ref, wv_ref, kv_ref, q_ref,
             xin, a, wkv, wqs, kvo, qo, local, pair_s, pair_r, kvg_s, kvg_r, qg_s, qg_r, kvs_s, kvs_r, kvz_s, kvz_r, dup_s, dup_r, qs_s, qs_r):
    me = lax.axis_index("sp")
    c, chip = lax.rem(me, 2), lax.div(me, 2)
    plane = lax.div(chip, 2)
    mate = flip(me, 1)
    oc = 1 - c
    rows = D // 16
    own = pl.ds(pl.multiple_of((2 * chip + c) * rows, 32), rows)
    mine = pl.ds(pl.multiple_of(c * OWN, OWN), OWN)
    meet(me)

    def pair(n, src, dst):
        return remote(src, dst, pair_s.at[n], pair_r.at[n], mate)

    def head_columns(g, core):
        return pl.ds(pl.multiple_of((2 * g + core) * HEAD, HEAD), HEAD)

    def kv_local(src):
        return pltpu.make_async_copy(src, wkv.at[own], local.at[0])

    @pl.when(c == 0)
    def _():
        pair(0, wv_ref, wkv.at[own]).start()
        kv_local(wk_ref).start()

    @pl.when(c == 1)
    def _():
        pair(0, wk_ref, wkv.at[own]).start()
        kv_local(wv_ref).start()

    pair_x = pair(1, x_ref, xin.at[mine])
    local_x = pltpu.make_async_copy(x_ref, xin.at[mine], local.at[1])
    pair_q = [pair(2 + g, wq_ref.at[:, head_columns(g, oc)], wqs.at[own, pl.ds(g * HEAD, HEAD)]) for g in range(4)]
    local_q = [pltpu.make_async_copy(wq_ref.at[:, head_columns(g, c)], wqs.at[own, pl.ds(g * HEAD, HEAD)], local.at[2 + g]) for g in range(4)]
    for copy in (pair_x, local_x, *pair_q, *local_q):
        copy.start()

    def rows_of(buf):
        return lambda q, first, n: buf.at[pl.ds(pl.multiple_of(q * (2 * rows) + first, 16), n)]

    thirds = ((0, 112), (112, 112), (224, 96))
    kvg = Gather(rows_of(wkv), thirds, me, kvg_s, kvg_r)
    qg = Gather(rows_of(wqs), thirds, me, qg_s, qg_r)

    kv_local(wk_ref).wait()
    pair(0, wk_ref, wkv.at[own]).wait_recv()
    kvg.start(0, 1, 3)

    pair_x.wait_recv()
    local_x.wait()

    def norm(r, _):
        here = pl.ds(pl.multiple_of(r * 64, 64), 64)
        wide = xin[here, :].astype(jnp.float32)
        scale = lax.rsqrt(jnp.mean(wide * wide, -1, keepdims=True) + 1e-6)
        a[here, :] = (wide * scale * gain_ref[...].astype(jnp.float32)).astype(jnp.bfloat16)

    half = TOK // 64 // 2
    lax.fori_loop(0, half, norm, None)
    kvg.arrived(0)
    kvg.start(2, 4)
    lax.fori_loop(half, 2 * half, norm, None)
    kvg.arrived(1)
    kvg.start(5)
    kvg.arrived(2)
    kvg.start(6)
    for copy in (*local_q,):
        copy.wait()
    for copy in (*pair_q,):
        copy.wait_recv()
    qg.start(0, 1, 3)
    kvg.arrived(3, 4, 5, 6)

    def turned_heads(w, out, g, plain):
        def body(r, _):
            here = pl.ds(pl.multiple_of(r * 512, 512), 512)
            t = dot(a[here, :], w[:, g * HEAD : (g + 1) * HEAD], 1, 0).astype(jnp.bfloat16).astype(jnp.float32)
            cos, sin = cos_ref[here, :], sin_ref[here, :]
            if plain is not None:
                cos, sin = jnp.where(plain == 1, 1.0, cos), jnp.where(plain == 1, 0.0, sin)
            p, q = t[:, : HEAD // 2], t[:, HEAD // 2 :]
            out[g, here, : HEAD // 2] = (p * cos - q * sin).astype(jnp.bfloat16)
            out[g, here, HEAD // 2 :] = (q * cos + p * sin).astype(jnp.bfloat16)

        lax.fori_loop(0, TOK // 512, body, None)

    for g in range(4):
        turned_heads(wkv, kvo, g, c)

    ways = ((), (X,), (Y,), (X, Y))

    def kv_send(n):
        return remote(kvo.at[lax.div(flip(chip, *ways[n]), 2)], kv_ref.at[c, chip], kvs_s.at[n], kvs_r.at[n], flip(me, *[2 * w for w in ways[n]]))

    keep_kv = pltpu.make_async_copy(kvo.at[plane], kv_ref.at[c, chip], local.at[6])
    keep_kv.start()
    for n in (3, 1, 2):
        kv_send(n).start()

    def kv_z(n):
        source = flip(chip, *ways[n])
        src = kvo.at[plane] if n == 0 else kv_ref.at[c, source]
        return remote(src, kv_ref.at[c, source], kvz_s.at[n], kvz_r.at[n], flip(me, 2 * Z))

    def dup(n):
        source = flip(chip, *ways[n % 4], *([Z] if n >= 4 else []))
        src = kvo.at[plane] if n == 0 else kv_ref.at[c, source]
        return remote(src, kv_ref.at[c, source], dup_s.at[n], dup_r.at[n], mate)

    kv_z(0).start()
    dup(0).start()

    qg.arrived(0)
    qg.start(2, 4)
    qg.arrived(1)
    qg.start(5)
    qg.arrived(2)
    qg.start(6)
    for n in (1, 2, 3):
        kv_send(n).wait_recv()
        kv_z(n).start()
        dup(n).start()
    qg.arrived(3, 4, 5, 6)

    for g in range(4):
        turned_heads(wqs, qo, g, None)

    def q_send(n):
        return remote(qo.at[lax.div(flip(chip, *ways[n]), 2)], q_ref.at[plane], qs_s.at[n], qs_r.at[n], flip(me, *[2 * w for w in ways[n]]))

    keep_q = pltpu.make_async_copy(qo.at[plane], q_ref.at[plane], local.at[7])
    keep_q.start()
    for n in (3, 1, 2):
        q_send(n).start()
    for n in range(4):
        kv_z(n).wait_recv()
        dup(4 + n).start()
    for n in (1, 2, 3):
        q_send(n).wait_recv()
    for n in range(8):
        dup(n).wait_recv()
    keep_kv.wait()
    keep_q.wait()
    pair(0, wk_ref, wkv.at[own]).wait_send()
    for copy in (pair_x, *pair_q):
        copy.wait_send()
    kvg.sent()
    qg.sent()
    for n in (1, 2, 3):
        kv_send(n).wait_send()
        q_send(n).wait_send()
    for n in range(4):
        kv_z(n).wait_send()
    for n in range(8):
        dup(n).wait_send()


def gather_project(x, gain, cos, sin, wq, wk, wv):
    bf, dma = jnp.bfloat16, pltpu.SemaphoreType.DMA
    hbm, vmem = pl.BlockSpec(memory_space=HBM), pl.BlockSpec(memory_space=pltpu.VMEM)
    return pl.pallas_call(
        _project,
        in_specs=[hbm, vmem, vmem, vmem, hbm, hbm, hbm],
        out_specs=[hbm, hbm],
        out_shape=[jax.ShapeDtypeStruct((2, CHIPS, TOK, HEAD), bf), jax.ShapeDtypeStruct((4, TOK, HEAD), bf)],
        scratch_shapes=[
            pltpu.VMEM((TOK, D), bf), pltpu.VMEM((TOK, D), bf), pltpu.VMEM((D, 1024), bf), pltpu.VMEM((D, 1024), bf),
            pltpu.VMEM((4, TOK, HEAD), bf), pltpu.VMEM((4, TOK, HEAD), bf),
            dma((8,)), dma((6,)), dma((6,)), dma((21,)), dma((21,)), dma((21,)), dma((21,)), dma((4,)), dma((4,)), dma((4,)), dma((4,)),
            dma((8,)), dma((8,)), dma((4,)), dma((4,)),
        ],
        compiler_params=pltpu.CompilerParams(collective_id=0, has_side_effects=True, vmem_limit_bytes=VMEM),
        cost_estimate=pl.CostEstimate(flops=2 * TOK * D * 2048, transcendentals=0, bytes_accessed=40 * 2**20),
    )(x, gain.reshape(1, D), cos, sin, wq, wk, wv)


def _attend(kv_ref, q_ref, wo_ref, seen_ref, full_ref, kbuf, vbuf, qbuf, obuf, top_s, mix_s, gap_s,
            local, kv_l, wg_s, wg_r, pair_s, pair_r, dup_s, dup_r, out_s, out_r):
    me = lax.axis_index("sp")
    c, chip = lax.rem(me, 2), lax.div(me, 2)
    plane, z = lax.div(chip, 2), lax.rem(chip, 2)
    mate = flip(me, 1)
    wrows = 128
    wown = pl.ds(pl.multiple_of(me * wrows, wrows), wrows)
    columns = pl.ds(pl.multiple_of(c * (D // 2), 128), D // 2)

    loads = [pltpu.make_async_copy(q_ref, qbuf, local.at[0])]
    for b in range(CHIPS):
        here = pl.ds(b * TOK, TOK)
        loads.append(pltpu.make_async_copy(kv_ref.at[0, b], kbuf.at[here], kv_l.at[2 * b]))
        loads.append(pltpu.make_async_copy(kv_ref.at[1, b], vbuf.at[here], kv_l.at[2 * b + 1]))
    for copy in loads:
        copy.start()
    meet(me)
    keep_w = pltpu.make_async_copy(wo_ref, full_ref.at[wown], local.at[1])
    keep_w.start()
    pair_w = remote(wo_ref, full_ref.at[wown], pair_s.at[0], pair_r.at[0], mate)
    pair_w.start()
    wg = Gather(lambda q, first, n: full_ref.at[pl.ds(pl.multiple_of(q * (2 * wrows) + first, 16), n), columns],
                ((0, 96), (96, 80), (176, 80)), me, wg_s, wg_r)

    def dup(i, s):
        view = wg.landed(i, s)
        return remote(view, view, dup_s.at[7 * i + s], dup_r.at[7 * i + s], mate)

    def duplicate(*sends):
        for s in sends:
            for i in range(3):
                dup(i, s).start()

    gap_s[...] = lax.broadcasted_iota(jnp.int32, (512, 512), 1) - lax.broadcasted_iota(jnp.int32, (512, 512), 0)
    e = HEAD**-0.5 * LOG2E
    ones = jnp.ones((8, 512), jnp.bfloat16)

    def scores(slot, strip, first, n):
        return dot(kbuf[pl.ds(first, n), :], qbuf[slot, strip * 512 : (strip + 1) * 512, :], 1, 1)

    def weigh(strip, s):
        at = pl.ds(strip * 512, 512)
        old = top_s[:, at]
        top = jnp.maximum(old, s.max(axis=0, keepdims=True))
        top_s[:, at] = top
        return jnp.exp2((s - top) * e).astype(jnp.bfloat16), jnp.exp2((old - top) * e)

    def add(strip, first, n, p, keep):
        at = pl.ds(strip * 512, 512)
        values = jnp.concatenate([vbuf[pl.ds(first, n), :].T, jnp.ones((8, n), jnp.bfloat16)], axis=0)
        mix_s[:, at] = mix_s[:, at] * keep + dot(values, p, 1, 0)

    def block(slot):
        last = 2 * slot + z
        top_s[...] = jnp.full(top_s.shape, NEG, jnp.float32)
        mix_s[...] = jnp.zeros(mix_s.shape, jnp.float32)

        def whole(j, _):
            first = pl.multiple_of(j * TOK, TOK)
            s = [scores(slot, n, first, TOK) for n in range(2)]
            w = [weigh(n, s[n]) for n in range(2)]
            for n in range(2):
                add(n, first, TOK, *w[n])

        lax.fori_loop(0, last, whole, None)
        first = pl.multiple_of(last * TOK, TOK)
        second = pl.multiple_of(last * TOK + 512, 512)
        ok = gap_s[...] >= 0
        s0 = jnp.where(ok, scores(slot, 0, first, 512), HIDDEN)
        s1 = scores(slot, 1, first, 512)
        s2 = jnp.where(ok, scores(slot, 1, second, 512), HIDDEN)
        w0, w1 = weigh(0, s0), weigh(1, s1)
        add(0, first, 512, *w0)
        add(1, first, 512, *w1)
        w2 = weigh(1, s2)
        add(1, second, 512, *w2)
        obuf[slot] = (mix_s[:HEAD, :] * (1 / mix_s[HEAD : HEAD + 1, :])).T.astype(jnp.bfloat16)

    ways = ((), (X,), (Y,), (X, Y))
    head = pl.ds(pl.multiple_of((2 * plane + c) * HEAD, HEAD), HEAD)

    def out(n, core):
        slot = lax.div(flip(chip, *ways[n]), 2)
        to = c if core == 0 else 1 - c
        device = flip(me, *[2 * w for w in ways[n]], *([1] if core else []))
        src = obuf.at[slot, pl.ds(pl.multiple_of(to * OWN, OWN), OWN)]
        if n == 0 and core == 0:
            return pltpu.make_async_copy(src, seen_ref.at[:, head], local.at[2])
        return remote(src, seen_ref.at[:, head], out_s.at[2 * n + core], out_r.at[2 * n + core], device)

    keep_w.wait()
    pair_w.wait_recv()
    wg.start(0, 1, 3)
    for copy in loads:
        copy.wait()

    block(lax.div(flip(chip, *ways[3]), 2))
    for core in range(2):
        out(3, core).start()
    wg.arrived(0)
    wg.start(2, 4)
    duplicate(0)
    wg.arrived(1)
    wg.start(5)
    duplicate(1)
    block(lax.div(flip(chip, *ways[1]), 2))
    for core in range(2):
        out(1, core).start()
    wg.arrived(2)
    wg.start(6)
    duplicate(2)
    block(lax.div(flip(chip, *ways[2]), 2))
    for core in range(2):
        out(2, core).start()
    wg.arrived(3, 4)
    duplicate(3, 4)
    block(plane)
    for core in range(2):
        out(0, core).start()
    wg.arrived(5, 6)
    duplicate(5, 6)
    out(0, 0).wait()
    for n in range(4):
        for core in range(2):
            if n or core:
                out(n, core).wait_recv()
    for s in range(7):
        for i in range(3):
            dup(i, s).wait_recv()
    pair_w.wait_send()
    wg.sent()
    for s in range(7):
        for i in range(3):
            dup(i, s).wait_send()
    for n in range(4):
        for core in range(2):
            if n or core:
                out(n, core).wait_send()


def attend_return(kv, q, wo):
    bf, dma = jnp.bfloat16, pltpu.SemaphoreType.DMA
    hbm = pl.BlockSpec(memory_space=HBM)
    return pl.pallas_call(
        _attend,
        in_specs=[hbm, hbm, hbm],
        out_specs=[hbm, hbm],
        out_shape=[jax.ShapeDtypeStruct((OWN, 2048), bf), jax.ShapeDtypeStruct((2048, D), bf)],
        scratch_shapes=[
            pltpu.VMEM((8192, HEAD), bf), pltpu.VMEM((8192, HEAD), bf), pltpu.VMEM((4, TOK, HEAD), bf), pltpu.VMEM((4, TOK, HEAD), bf),
            pltpu.VMEM((1, TOK), jnp.float32), pltpu.VMEM((HEAD + 8, TOK), jnp.float32), pltpu.VMEM((512, 512), jnp.int32),
            dma((3,)), dma((16,)), dma((21,)), dma((21,)), dma((1,)), dma((1,)), dma((21,)), dma((21,)), dma((8,)), dma((8,)),
        ],
        compiler_params=pltpu.CompilerParams(collective_id=1, has_side_effects=True, vmem_limit_bytes=VMEM),
        cost_estimate=pl.CostEstimate(flops=4 * 18 * TOK * TOK * HEAD, transcendentals=18 * TOK * TOK, bytes_accessed=40 * 2**20),
    )(kv, q, wo)


def solution(mesh):
    def step(x, gain, wq, wk, wv, wo):
        chip = lax.div(lax.axis_index("sp"), 2)
        place = chip * TOK + jnp.arange(TOK)
        half = HEAD // 2
        angle = place.astype(jnp.float32)[:, None] * THETA ** (-jnp.arange(half, dtype=jnp.float32) / half)
        kv, q = gather_project(x, gain, jnp.cos(angle), jnp.sin(angle), wq, wk, wv)
        seen, full = attend_return(kv, q, wo)
        y = jnp.dot(seen, full, preferred_element_type=jnp.float32)
        return (x.astype(jnp.float32) + y).astype(jnp.bfloat16)

    tokens, whole = P(("dp", "sp"), None), P("sp", None)
    return jax.shard_map(
        step,
        mesh=mesh,
        in_specs=(tokens, P(None), whole, whole, whole, whole),
        out_specs=tokens,
        check_vma=False,
    )
```

```python
import jax
import jax.numpy as jnp
from jax import lax
from jax.experimental import pallas as pl
from jax.experimental.pallas import tpu as pltpu
from jax.sharding import PartitionSpec as P

HEAD = 256
THETA = 10000
D = 2560
OWN = 512
TOK = 1024
NEG = -1e30
HIDDEN = 2 * NEG
LOG2E = 1.4426950408889634
VMEM = 63 * 2**20
MESH = pl.DeviceIdType.MESH
HBM = pltpu.HBM
X, Y, Z, C = 8, 4, 2, 1
ROWS = D // 16
SENDS = ((0, ()), (1, ()), (1, (0,)), (2, ()), (2, (0,)), (2, (1,)), (2, (0, 1)))
PIECES = ((0, 0, 0, 512), (0, 1, 0, 512), (1, 0, 0, 256), (1, 1, 0, 256), (1, 0, 256, 256), (1, 1, 256, 256))


def flip(v, *bits):
    out = v
    for w in bits:
        out = out + w * (1 - 2 * lax.rem(lax.div(v, w), 2))
    return out


def remote(src, dst, send, recv, device):
    return pltpu.make_async_remote_copy(src_ref=src, dst_ref=dst, send_sem=send, recv_sem=recv, device_id={"sp": device}, device_id_type=MESH)


def dot(a, b, ca, cb):
    return lax.dot_general(a, b, (((ca,), (cb,)), ((), ())), preferred_element_type=jnp.float32)


class Gather:
    def __init__(self, view, orders, me, send_sem, recv_sem):
        self.view, self.orders, self.me, self.send_sem, self.recv_sem = view, orders, me, send_sem, recv_sem
        self.n = 2 ** len(orders[0]) - 1
        self.parts = range(len(orders))

    def copy(self, i, s):
        order = self.orders[i]
        link, path = SENDS[s]
        view = self.view(i, flip(self.me, *[order[k] for k in path]))
        return remote(view, view, self.send_sem.at[self.n * i + s], self.recv_sem.at[self.n * i + s], flip(self.me, order[link]))

    def landed(self, i, s):
        order = self.orders[i]
        link, path = SENDS[s]
        return self.view(i, flip(self.me, order[link], *[order[k] for k in path]))

    def start(self, sends, parts=None):
        for s in sends:
            for i in self.parts if parts is None else parts:
                self.copy(i, s).start()

    def arrived(self, sends, parts=None):
        for s in sends:
            for i in self.parts if parts is None else parts:
                self.copy(i, s).wait_recv()

    def sent(self):
        for i in self.parts:
            for s in range(self.n):
                self.copy(i, s).wait_send()


def _layer(x_ref, gain_ref, freq_ref, wq_ref, wk_ref, wv_ref, wo_ref, seen_ref, full_ref,
           xin, a, wkv, wqs, kv2, kvy, qbuf, qy, obuf, cos_s, sin_s, top_s, mix_s, gap_s,
           local, wi_s, wi_r, kvg_s, kvg_r, qg_s, qg_r, ax_s, ax_r, am_s, am_r, ky_s, ky_r, qy_s, qy_r, kz_s, kz_r, dup_s, dup_r,
           wp_s, wp_r, wg_s, wg_r, wd_s, wd_r, out_s, out_r):
    me = lax.axis_index("sp")
    c, z, y, x = lax.rem(me, 2), lax.rem(lax.div(me, 2), 2), lax.rem(lax.div(me, 4), 2), lax.div(me, 8)
    mate = flip(me, C)
    own_rows = pl.ds(pl.multiple_of(me * ROWS, 32), ROWS)

    barrier = pltpu.get_barrier_semaphore()
    for mask in range(1, 16):
        pl.semaphore_signal(barrier, inc=1, device_id={"sp": flip(me, *[w for w in (1, 2, 4, 8) if mask & w])}, device_id_type=MESH)
    load_x = pltpu.make_async_copy(x_ref, xin, local.at[0])
    load_x.start()
    pl.semaphore_wait(barrier, 15)

    TO = ((), (C,), (X,), (X, C))

    def kv_first(rel, src):
        target = flip(me, *TO[rel])
        cols = pl.ds(pl.multiple_of(lax.div(target, 8) * 512, 512), 512)
        if rel == 0:
            return pltpu.make_async_copy(src.at[:, cols], wkv.at[own_rows], local.at[1])
        return remote(src.at[:, cols], wkv.at[own_rows], wi_s.at[rel - 1], wi_r.at[rel - 1], target)

    def q_first(rel, j):
        target = flip(me, *TO[rel])
        head = 4 * lax.div(target, 8) + 2 * j + lax.rem(target, 2)
        cols = pl.ds(pl.multiple_of(head * HEAD, HEAD), HEAD)
        dst = wqs.at[own_rows, pl.ds(j * HEAD, HEAD)]
        if rel == 0:
            return pltpu.make_async_copy(wq_ref.at[:, cols], dst, local.at[2 + j])
        n = 3 + 2 * (rel - 1) + j
        return remote(wq_ref.at[:, cols], dst, wi_s.at[n], wi_r.at[n], target)

    @pl.when(c == 0)
    def _():
        for rel, src in ((1, wv_ref), (0, wk_ref), (2, wk_ref), (3, wv_ref)):
            kv_first(rel, src).start()

    @pl.when(c == 1)
    def _():
        for rel, src in ((1, wk_ref), (0, wv_ref), (2, wv_ref), (3, wk_ref)):
            kv_first(rel, src).start()

    for rel in (1, 0, 2, 3):
        for j in range(2):
            q_first(rel, j).start()

    def rows_of(buf):
        def view(i, device):
            chip = lax.div(flip(device, X) if i else device, 2)
            return buf.at[pl.ds(pl.multiple_of(chip * (2 * ROWS), 64), 2 * ROWS)]
        return view

    kvg = Gather(rows_of(wkv), ((Y, Z), (Z, Y)), me, kvg_s, kvg_r)
    qg = Gather(rows_of(wqs), ((Y, Z), (Z, Y)), me, qg_s, qg_r)

    def quarter(fx, fc):
        return 2 * lax.div(flip(me, *([X] if fx else [])), 8) + lax.rem(flip(me, *([C] if fc else [])), 2)

    mine = quarter(0, 0)

    def a_view(h):
        return a.at[mine, pl.ds(h * 256, 256)]

    def a_mate(h):
        return remote(a_view(h), a_view(h), am_s.at[h], am_r.at[h], mate)

    def a_x(h):
        return remote(a_view(h), a_view(h), ax_s.at[h], ax_r.at[h], flip(me, X))

    def a_pass(h):
        view = a.at[quarter(1, 0), pl.ds(h * 256, 256)]
        return remote(view, view, am_s.at[2 + h], am_r.at[2 + h], mate)

    gain = gain_ref[...].astype(jnp.float32).reshape(1, D)

    def norm(r, _):
        here = pl.ds(pl.multiple_of(r * 64, 64), 64)
        wide = xin[here, :].astype(jnp.float32)
        scale = lax.rsqrt(jnp.mean(wide * wide, -1, keepdims=True) + 1e-6)
        a[mine, here, :] = (wide * scale * gain).astype(jnp.bfloat16)

    kv_first(0, wk_ref).wait()
    kv_first(1, wk_ref).wait_recv()
    kvg.start((0, 1), (0,))
    load_x.wait()
    for h in range(2):
        lax.fori_loop(4 * h, 4 * h + 4, norm, None)
        a_x(h).start()
        a_mate(h).start()
    kv_first(2, wk_ref).wait_recv()
    kv_first(3, wk_ref).wait_recv()
    kvg.start((0, 1), (1,))
    for j in range(2):
        q_first(0, j).wait()
        q_first(1, j).wait_recv()
    kvg.arrived((0,), (0,))
    kvg.start((2,), (0,))
    kvg.arrived((0,), (1,))
    kvg.start((2,), (1,))
    qg.start((0, 1), (0,))
    for j in range(2):
        q_first(2, j).wait_recv()
        q_first(3, j).wait_recv()
    qg.start((0, 1), (1,))
    wown = pl.ds(pl.multiple_of(me * 128, 128), 128)
    keep_w = pltpu.make_async_copy(wo_ref, full_ref.at[wown], local.at[4])
    pair_w = remote(wo_ref, full_ref.at[wown], wp_s.at[0], wp_r.at[0], mate)
    keep_w.start()
    pair_w.start()

    for fx in range(2):
        for fc in range(2):
            n = quarter(fx, fc)
            token = 512 * flip(me, *([X] if fx else []), *([C] if fc else []))

            def angles(r, _):
                here = pl.ds(pl.multiple_of(r * 64, 64), 64)
                place = (token + r * 64 + lax.broadcasted_iota(jnp.int32, (64, HEAD // 2), 0)).astype(jnp.float32)
                angle = place * freq_ref[...]
                cos_s[n, here, :] = jnp.cos(angle)
                sin_s[n, here, :] = jnp.sin(angle)

            lax.fori_loop(0, 8, angles, None)

    def turned(w, piece, head, plain, out):
        fx, fc, first, n = PIECES[piece]
        t4 = quarter(fx, fc)
        cols = pl.ds(pl.multiple_of(head * HEAD, HEAD), HEAD)

        def body(r, _):
            here = pl.ds(pl.multiple_of(first + r * 256, 256), 256)
            t = dot(a[t4, here, :], w[:, cols], 1, 0).astype(jnp.bfloat16).astype(jnp.float32)
            cos, sin = cos_s[t4, here, :], sin_s[t4, here, :]
            if plain is not None:
                cos, sin = jnp.where(plain == 1, 1.0, cos), jnp.where(plain == 1, 0.0, sin)
            p, q = t[:, : HEAD // 2], t[:, HEAD // 2 :]
            out(r, (p * cos - q * sin).astype(jnp.bfloat16), (q * cos + p * sin).astype(jnp.bfloat16))

        lax.fori_loop(0, n // 256, body, None)

    def token_rows(piece, *bits):
        fx, fc, first, n = PIECES[piece]
        device = flip(me, *([X] if fx else []), *([C] if fc else []), *bits)
        return pl.ds(pl.multiple_of(device * OWN + first, 256), n)

    def kv_view(piece, *bits):
        return kv2.at[c, token_rows(piece, *bits)]

    def stage(buf, piece):
        fx, fc, first, n = PIECES[piece]
        return buf.at[pl.ds(pl.multiple_of(quarter(fx, fc) * OWN + first, 256), n)]

    def q_view(piece, *bits):
        fx, fc, first, n = PIECES[piece]
        device = flip(me, *([X] if fx else []), *([C] if fc else []), *bits)
        slot = 4 * lax.div(device, 8) + 2 * lax.rem(lax.div(device, 4), 2) + lax.rem(device, 2)
        return qbuf.at[pl.ds(pl.multiple_of(slot * OWN + first, 256), n)]

    def write(view):
        def out(r, left, right):
            view[pl.ds(pl.multiple_of(r * 256, 256), 256), : HEAD // 2] = left
            view[pl.ds(pl.multiple_of(r * 256, 256), 256), HEAD // 2 :] = right
        return out

    def kv_y(piece):
        return remote(stage(kvy, piece), kv_view(piece), ky_s.at[piece], ky_r.at[piece], flip(me, Y))

    def q_y(piece):
        return remote(stage(qy, piece), q_view(piece), qy_s.at[piece], qy_r.at[piece], flip(me, Y))

    def kv_z(n):
        view = kv_view(n % 6, *([Y] if n >= 6 else []))
        return remote(view, view, kz_s.at[n], kz_r.at[n], flip(me, Z))

    def dup(n):
        view = kv_view(n % 6, *([Y] if n % 12 >= 6 else []), *([Z] if n >= 12 else []))
        return remote(view, view, dup_s.at[n], dup_r.at[n], mate)

    def project_kv(piece):
        turned(wkv, piece, 1 - y, c, write(stage(kvy, piece)))
        kv_y(piece).start()
        turned(wkv, piece, y, c, write(kv_view(piece)))
        kv_z(piece).start()
        dup(piece).start()

    def project_q(piece):
        turned(wqs, piece, 1 - y, None, write(stage(qy, piece)))
        q_y(piece).start()
        turned(wqs, piece, y, None, write(q_view(piece)))

    def pass_y(piece):
        kv_y(piece).wait_recv()
        kv_z(6 + piece).start()
        dup(6 + piece).start()

    def pass_z(n):
        kv_z(n).wait_recv()
        dup(12 + n).start()

    kvg.arrived((1, 2))
    a_mate(0).wait_recv()
    a_mate(1).wait_recv()
    project_kv(0)
    qg.arrived((0,))
    qg.start((2,))
    project_kv(1)
    pass_y(0)
    pass_y(1)
    qg.arrived((1, 2))
    project_q(0)
    project_q(1)

    columns = pl.ds(pl.multiple_of(c * (D // 2), 128), D // 2)
    wg = Gather(lambda i, device: full_ref.at[pl.ds(pl.multiple_of(lax.div(device, 2) * 256 + i * 128, 128), 128), columns],
                ((Y, X, Z), (Y, Z, X)), me, wg_s, wg_r)

    def wdup(i, s):
        view = wg.landed(i, s)
        return remote(view, view, wd_s.at[7 * i + s], wd_r.at[7 * i + s], mate)

    def duplicate(*sends):
        for s in sends:
            for i in range(2):
                wdup(i, s).start()

    keep_w.wait()
    pair_w.wait_recv()
    wg.start((0,))
    wg.start((1,), (0,))
    wg.start((3,), (1,))
    for h in range(2):
        a_x(h).wait_recv()
        a_pass(h).start()
        project_kv(2 + 2 * h)
        project_q(2 + 2 * h)
        a_pass(h).wait_recv()
        project_kv(3 + 2 * h)
        project_q(3 + 2 * h)
        pass_y(2 + 2 * h)
        pass_y(3 + 2 * h)
    wg.start((1,), (1,))
    wg.start((3,), (0,))
    wg.arrived((0,))
    wg.start((2, 4))
    duplicate(0)
    for n in range(12):
        pass_z(n)
    for piece in range(6):
        q_y(piece).wait_recv()
    for n in range(24):
        dup(n).wait_recv()

    gap_s[...] = lax.broadcasted_iota(jnp.int32, (512, 512), 1) - lax.broadcasted_iota(jnp.int32, (512, 512), 0)
    e = HEAD**-0.5 * LOG2E

    def scores(strip, at, first, n):
        return dot(kv2[0, pl.ds(first, n), :], qbuf[pl.ds(pl.multiple_of(at + strip * 512, 512), 512), :], 1, 1)

    def weigh(strip, s):
        at = pl.ds(strip * 512, 512)
        old = top_s[:, at]
        top = jnp.maximum(old, s.max(axis=0, keepdims=True))
        top_s[:, at] = top
        return jnp.exp2((s - top) * e).astype(jnp.bfloat16), jnp.exp2((old - top) * e)

    def add(strip, first, n, p, keep):
        at = pl.ds(strip * 512, 512)
        values = jnp.concatenate([kv2[1, pl.ds(first, n), :].T, jnp.ones((8, n), jnp.bfloat16)], axis=0)
        mix_s[:, at] = mix_s[:, at] * keep + dot(values, p, 1, 0)

    def poll_1():
        wg.arrived((1,))
        wg.start((5,))
        duplicate(1)

    def poll_2():
        wg.arrived((2,))
        wg.start((6,))
        duplicate(2)

    def poll_3():
        wg.arrived((3, 4))
        duplicate(3, 4)

    polls = ((2, poll_1), (5, poll_2), (11, poll_3))
    head = pl.ds(pl.multiple_of((2 * (2 * x + y) + c) * HEAD, HEAD), HEAD)

    def out(i, core):
        fx, fy = lax.div(3 - i, 2), lax.rem(3 - i, 2)
        x2, y2 = x + fx * (1 - 2 * x), y + fy * (1 - 2 * y)
        to = c if core == 0 else 1 - c
        device = 8 * x2 + 4 * y2 + 2 * z + to
        src = obuf.at[pl.ds(pl.multiple_of((2 * x2 + y2) * TOK + to * OWN, OWN), OWN)]
        return src, device, 2 * i + core

    def out_far(i, core):
        src, device, n = out(i, core)
        return remote(src, seen_ref.at[:, head], out_s.at[n], out_r.at[n], device)

    def out_here():
        src, _, _ = out(3, 0)
        return pltpu.make_async_copy(src, seen_ref.at[:, head], local.at[5])

    def block(i, count):
        fx, fy = lax.div(3 - i, 2), lax.rem(3 - i, 2)
        slot = 2 * (x + fx * (1 - 2 * x)) + y + fy * (1 - 2 * y)
        at = slot * TOK
        last = 2 * slot + z
        top_s[...] = jnp.full(top_s.shape, NEG, jnp.float32)
        mix_s[...] = jnp.zeros(mix_s.shape, jnp.float32)

        def whole(j, _):
            first = pl.multiple_of(j * TOK, TOK)
            s = [scores(n, at, first, TOK) for n in range(2)]
            w = [weigh(n, s[n]) for n in range(2)]
            for n in range(2):
                add(n, first, TOK, *w[n])
            for when, what in polls:
                pl.when(count + j == when)(what)

        lax.fori_loop(0, last, whole, None)
        first = pl.multiple_of(last * TOK, TOK)
        second = pl.multiple_of(last * TOK + 512, 512)
        ok = gap_s[...] >= 0
        s0 = jnp.where(ok, scores(0, at, first, 512), HIDDEN)
        s1 = scores(1, at, first, 512)
        s2 = jnp.where(ok, scores(1, at, second, 512), HIDDEN)
        w0, w1 = weigh(0, s0), weigh(1, s1)
        add(0, first, 512, *w0)
        add(1, first, 512, *w1)
        w2 = weigh(1, s2)
        add(1, second, 512, *w2)
        obuf[pl.ds(pl.multiple_of(at, TOK), TOK), :] = (mix_s[:HEAD, :] * (1 / mix_s[HEAD : HEAD + 1, :])).T.astype(jnp.bfloat16)

        @pl.when(i < 3)
        def _():
            out_far(i, 0).start()

        out_far(i, 1).start()
        return count + last

    lax.fori_loop(0, 4, block, jnp.int32(0))
    out_here().start()
    wg.arrived((5, 6))
    duplicate(5, 6)
    out_here().wait()
    for i in range(4):
        for core in range(2):
            if i < 3 or core:
                out_far(i, core).wait_recv()
    for s in range(7):
        for i in range(2):
            wdup(i, s).wait_recv()

    for rel in (1, 2, 3):
        kv_first(rel, wk_ref).wait_send()
        for j in range(2):
            q_first(rel, j).wait_send()
    kvg.sent()
    qg.sent()
    for h in range(2):
        a_mate(h).wait_send()
        a_x(h).wait_send()
        a_pass(h).wait_send()
    for piece in range(6):
        kv_y(piece).wait_send()
        q_y(piece).wait_send()
    for n in range(12):
        kv_z(n).wait_send()
    for n in range(24):
        dup(n).wait_send()
    pair_w.wait_send()
    wg.sent()
    for s in range(7):
        for i in range(2):
            wdup(i, s).wait_send()
    for i in range(4):
        for core in range(2):
            if i < 3 or core:
                out_far(i, core).wait_send()


def attend_all(x, gain, freq, wq, wk, wv, wo):
    bf, f32 = jnp.bfloat16, jnp.float32
    hbm, vmem = pl.BlockSpec(memory_space=HBM), pl.BlockSpec(memory_space=pltpu.VMEM)
    sems = (6, 9, 9, 6, 6, 6, 6, 2, 2, 4, 4, 6, 6, 6, 6, 12, 12, 24, 24, 1, 1, 14, 14, 14, 14, 8, 8)
    return pl.pallas_call(
        _layer,
        in_specs=[hbm, vmem, vmem, hbm, hbm, hbm, hbm],
        out_specs=[hbm, hbm],
        out_shape=[jax.ShapeDtypeStruct((OWN, 2048), bf), jax.ShapeDtypeStruct((2048, D), bf)],
        scratch_shapes=[
            pltpu.VMEM((OWN, D), bf), pltpu.VMEM((4, OWN, D), bf), pltpu.VMEM((D, 512), bf), pltpu.VMEM((D, 512), bf),
            pltpu.VMEM((2, 8192, HEAD), bf), pltpu.VMEM((2048, HEAD), bf), pltpu.VMEM((4096, HEAD), bf), pltpu.VMEM((2048, HEAD), bf),
            pltpu.VMEM((4096, HEAD), bf), pltpu.VMEM((4, OWN, HEAD // 2), f32), pltpu.VMEM((4, OWN, HEAD // 2), f32),
            pltpu.VMEM((1, TOK), f32), pltpu.VMEM((HEAD + 8, TOK), f32), pltpu.VMEM((512, 512), jnp.int32),
            *[pltpu.SemaphoreType.DMA((n,)) for n in sems],
        ],
        compiler_params=pltpu.CompilerParams(collective_id=0, has_side_effects=True, vmem_limit_bytes=VMEM),
        cost_estimate=pl.CostEstimate(flops=2 * 2048 * D * 1024 + 4 * 18 * TOK * TOK * HEAD, transcendentals=18 * TOK * TOK, bytes_accessed=40 * 2**20),
    )(x, gain, freq, wq, wk, wv, wo)


def solution(mesh):
    def step(x, gain, wq, wk, wv, wo):
        half = HEAD // 2
        freq = (THETA ** (-jnp.arange(half, dtype=jnp.float32) / half)).reshape(1, half)
        seen, full = attend_all(x, gain, freq, wq, wk, wv, wo)
        y = jnp.dot(seen, full, preferred_element_type=jnp.float32)
        return (x.astype(jnp.float32) + y).astype(jnp.bfloat16)

    tokens, whole = P(("dp", "sp"), None), P("sp", None)
    return jax.shard_map(
        step,
        mesh=mesh,
        in_specs=(tokens, P(None), whole, whole, whole, whole),
        out_specs=tokens,
        check_vma=False,
    )
```

```python
import jax
import jax.numpy as jnp
from jax import lax
from jax.experimental import pallas as pl
from jax.experimental.pallas import tpu as pltpu
from jax.sharding import PartitionSpec as P

HEAD = 256
HALF = HEAD // 2
THETA = 10000
D = 2560
OWN = 512
TOK = 1024
NEG = -1e30
HIDDEN = 2 * NEG
LOG2E = 1.4426950408889634
LOCAL = 16
SEMS = LOCAL + 2 * (9 + 6 + 6 + 2 + 4 + 6 + 6 + 12 + 24 + 1 + 14 + 14 + 8)
STRIP = 256
VMEM = 67043328
MESH = pl.DeviceIdType.MESH
HBM = pltpu.HBM
X, Y, Z, C = 8, 4, 2, 1
ROWS = D // 16
SENDS = ((0, ()), (1, ()), (1, (0,)), (2, ()), (2, (0,)), (2, (1,)), (2, (0, 1)))
PIECES = (*((0, core, 0, OWN) for core in (0, 1)), *((1, core, first, STRIP) for first in (0, STRIP) for core in (0, 1)))


def flip(v, *bits):
    out = v
    for w in bits:
        out = out + w * (1 - 2 * lax.rem(lax.div(v, w), 2))
    return out


def remote(src, dst, send, recv, device):
    return pltpu.make_async_remote_copy(src_ref=src, dst_ref=dst, send_sem=send, recv_sem=recv, device_id={"sp": device}, device_id_type=MESH)


def dot(a, b, ca, cb):
    return lax.dot_general(a, b, (((ca,), (cb,)), ((), ())), preferred_element_type=jnp.float32)


class Gather:
    def __init__(self, view, orders, me, send_sem, recv_sem):
        self.view, self.orders, self.me, self.send_sem, self.recv_sem = view, orders, me, send_sem, recv_sem
        self.n = 2 ** len(orders[0]) - 1
        self.parts = range(len(orders))

    def copy(self, i, s):
        order = self.orders[i]
        link, path = SENDS[s]
        view = self.view(i, flip(self.me, *[order[k] for k in path]))
        return remote(view, view, self.send_sem.at[self.n * i + s], self.recv_sem.at[self.n * i + s], flip(self.me, order[link]))

    def landed(self, i, s):
        order = self.orders[i]
        link, path = SENDS[s]
        return self.view(i, flip(self.me, order[link], *[order[k] for k in path]))

    def start(self, sends, parts=None):
        for s in sends:
            for i in self.parts if parts is None else parts:
                self.copy(i, s).start()

    def arrived(self, sends, parts=None):
        for s in sends:
            for i in self.parts if parts is None else parts:
                self.copy(i, s).wait_recv()

    def sent(self):
        for i in self.parts:
            for s in range(self.n):
                self.copy(i, s).wait_send()


def _layer(x_ref, gain_ref, freq_ref, wq_ref, wk_ref, wv_ref, wo_ref, xin,
           a, wkv, wqs, kv2, kvy, qbuf, qy, wo, seen, cos_s, sin_s, state, sems):
    used = [0]

    def take(n):
        first = used[0]
        used[0] += n
        return sems.at[pl.ds(first, n)]

    local = take(LOCAL)
    wi_s, wi_r, kvg_s, kvg_r, qg_s, qg_r, ax_s, ax_r, am_s, am_r = (take(n) for n in (9, 6, 6, 2, 4) for _ in range(2))
    ky_s, ky_r, qy_s, qy_r, kz_s, kz_r, dup_s, dup_r = (take(n) for n in (6, 6, 12, 24) for _ in range(2))
    wp_s, wp_r, wg_s, wg_r, wd_s, wd_r, out_s, out_r = (take(n) for n in (1, 14, 14, 8) for _ in range(2))
    me = lax.axis_index("sp")
    c, z, y, x = lax.rem(me, 2), lax.rem(lax.div(me, 2), 2), lax.rem(lax.div(me, 4), 2), lax.div(me, 8)
    mate = flip(me, C)
    own_rows = pl.ds(pl.multiple_of(me * ROWS, 32), ROWS)

    barrier = pltpu.get_barrier_semaphore()
    for mask in range(1, 16):
        pl.semaphore_signal(barrier, inc=1, device_id={"sp": flip(me, *[w for w in (1, 2, 4, 8) if mask & w])}, device_id_type=MESH)
    load_x = pltpu.make_async_copy(x_ref, xin, local.at[0])
    load_x.start()
    pl.semaphore_wait(barrier, 15)

    TO = ((), (C,), (X,), (X, C))

    def kv_first(rel, src):
        target = flip(me, *TO[rel])
        cols = pl.ds(pl.multiple_of(lax.div(target, 8) * 512, 512), 512)
        if rel == 0:
            return pltpu.make_async_copy(src.at[:, cols], wkv.at[own_rows], local.at[1])
        return remote(src.at[:, cols], wkv.at[own_rows], wi_s.at[rel - 1], wi_r.at[rel - 1], target)

    def q_first(rel, j):
        target = flip(me, *TO[rel])
        head = 4 * lax.div(target, 8) + 2 * j + lax.rem(target, 2)
        cols = pl.ds(pl.multiple_of(head * HEAD, HEAD), HEAD)
        dst = wqs.at[own_rows, pl.ds(j * HEAD, HEAD)]
        if rel == 0:
            return pltpu.make_async_copy(wq_ref.at[:, cols], dst, local.at[2 + j])
        n = 3 + 2 * (rel - 1) + j
        return remote(wq_ref.at[:, cols], dst, wi_s.at[n], wi_r.at[n], target)

    @pl.when(c == 0)
    def _():
        for rel, src in ((1, wv_ref), (0, wk_ref), (2, wk_ref), (3, wv_ref)):
            kv_first(rel, src).start()

    @pl.when(c == 1)
    def _():
        for rel, src in ((1, wk_ref), (0, wv_ref), (2, wv_ref), (3, wk_ref)):
            kv_first(rel, src).start()

    for rel in (1, 0, 2, 3):
        for j in range(2):
            q_first(rel, j).start()

    def rows_of(buf):
        def view(i, device):
            chip = lax.div(flip(device, X) if i else device, 2)
            return buf.at[pl.ds(pl.multiple_of(chip * (2 * ROWS), 64), 2 * ROWS)]
        return view

    kvg = Gather(rows_of(wkv), ((Y, Z), (Z, Y)), me, kvg_s, kvg_r)
    qg = Gather(rows_of(wqs), ((Y, Z), (Z, Y)), me, qg_s, qg_r)

    def quarter(fx, fc):
        return 2 * lax.div(flip(me, *([X] if fx else [])), 8) + lax.rem(flip(me, *([C] if fc else [])), 2)

    mine = quarter(0, 0)

    def a_view(h):
        return a.at[mine, pl.ds(h * 256, 256)]

    def a_mate(h):
        return remote(a_view(h), a_view(h), am_s.at[h], am_r.at[h], mate)

    def a_x(h):
        return remote(a_view(h), a_view(h), ax_s.at[h], ax_r.at[h], flip(me, X))

    def a_pass(h):
        view = a.at[quarter(1, 0), pl.ds(h * 256, 256)]
        return remote(view, view, am_s.at[2 + h], am_r.at[2 + h], mate)

    gain = gain_ref[...].astype(jnp.float32).reshape(1, D)

    def norm(r, _):
        here = pl.ds(pl.multiple_of(r * 64, 64), 64)
        wide = xin[here, :].astype(jnp.float32)
        scale = lax.rsqrt(jnp.mean(wide * wide, -1, keepdims=True) + 1e-6)
        a[mine, here, :] = (wide * scale * gain).astype(jnp.bfloat16)

    kv_first(0, wk_ref).wait()
    kv_first(1, wk_ref).wait_recv()
    kvg.start((0, 1), (0,))
    load_x.wait()
    for h in range(2):
        lax.fori_loop(4 * h, 4 * h + 4, norm, None)
        a_x(h).start()
        a_mate(h).start()
    kv_first(2, wk_ref).wait_recv()
    kv_first(3, wk_ref).wait_recv()
    kvg.start((0, 1), (1,))
    for j in range(2):
        q_first(0, j).wait()
        q_first(1, j).wait_recv()
    kvg.arrived((0,), (0,))
    kvg.start((2,), (0,))
    kvg.arrived((0,), (1,))
    kvg.start((2,), (1,))
    qg.start((0, 1), (0,))
    for j in range(2):
        q_first(2, j).wait_recv()
        q_first(3, j).wait_recv()
    qg.start((0, 1), (1,))
    wown = pl.ds(pl.multiple_of(me * 128, 128), 128)
    keep_w = pltpu.make_async_copy(wo_ref, wo.at[wown], local.at[4])
    pair_w = remote(wo_ref, wo.at[wown], wp_s.at[0], wp_r.at[0], mate)
    keep_w.start()
    pair_w.start()

    for fx in range(2):
        for fc in range(2):
            n = quarter(fx, fc)
            token = 512 * flip(me, *([X] if fx else []), *([C] if fc else []))

            def angles(r, _):
                here = pl.ds(pl.multiple_of(r * 64, 64), 64)
                place = (token + r * 64 + lax.broadcasted_iota(jnp.int32, (64, HALF), 0)).astype(jnp.float32)
                angle = place * freq_ref[...]
                cos_s[n, here, :] = jnp.cos(angle)
                sin_s[n, here, :] = jnp.sin(angle)

            lax.fori_loop(0, 8, angles, None)

    def turned(w, piece, head, plain, out):
        fx, fc, first, n = PIECES[piece]
        t4 = quarter(fx, fc)
        cols = pl.ds(pl.multiple_of(head * HEAD, HEAD), HEAD)

        def body(r, _):
            here = pl.ds(pl.multiple_of(first + r * 256, 256), 256)
            t = dot(a[t4, here, :], w[:, cols], 1, 0).astype(jnp.bfloat16).astype(jnp.float32)
            cos, sin = cos_s[t4, here, :], sin_s[t4, here, :]
            if plain is not None:
                cos, sin = jnp.where(plain == 1, 1.0, cos), jnp.where(plain == 1, 0.0, sin)
            p, q = t[:, : HALF], t[:, HALF :]
            out(r, (p * cos - q * sin).astype(jnp.bfloat16), (q * cos + p * sin).astype(jnp.bfloat16))

        lax.fori_loop(0, n // 256, body, None)

    def token_rows(piece, *bits):
        fx, fc, first, n = PIECES[piece]
        device = flip(me, *([X] if fx else []), *([C] if fc else []), *bits)
        return pl.ds(pl.multiple_of(device * OWN + first, 256), n)

    def kv_view(piece, *bits):
        return kv2.at[c, token_rows(piece, *bits)]

    def stage(buf, piece):
        fx, fc, first, n = PIECES[piece]
        return buf.at[pl.ds(pl.multiple_of(quarter(fx, fc) * OWN + first, 256), n)]

    def q_view(piece, *bits):
        fx, fc, first, n = PIECES[piece]
        device = flip(me, *([X] if fx else []), *([C] if fc else []), *bits)
        slot = 4 * lax.div(device, 8) + 2 * lax.rem(lax.div(device, 4), 2) + lax.rem(device, 2)
        return qbuf.at[pl.ds(pl.multiple_of(slot * OWN + first, 256), n)]

    def write(view):
        def out(r, left, right):
            view[pl.ds(pl.multiple_of(r * 256, 256), 256), : HALF] = left
            view[pl.ds(pl.multiple_of(r * 256, 256), 256), HALF :] = right
        return out

    def kv_y(piece):
        return remote(stage(kvy, piece), kv_view(piece), ky_s.at[piece], ky_r.at[piece], flip(me, Y))

    def q_y(piece):
        return remote(stage(qy, piece), q_view(piece), qy_s.at[piece], qy_r.at[piece], flip(me, Y))

    def kv_z(n):
        view = kv_view(n % 6, *([Y] if n >= 6 else []))
        return remote(view, view, kz_s.at[n], kz_r.at[n], flip(me, Z))

    def dup(n):
        view = kv_view(n % 6, *([Y] if n % 12 >= 6 else []), *([Z] if n >= 12 else []))
        return remote(view, view, dup_s.at[n], dup_r.at[n], mate)

    def project_kv(piece):
        turned(wkv, piece, 1 - y, c, write(stage(kvy, piece)))
        kv_y(piece).start()
        turned(wkv, piece, y, c, write(kv_view(piece)))
        kv_z(piece).start()
        dup(piece).start()

    def project_q(piece):
        turned(wqs, piece, 1 - y, None, write(stage(qy, piece)))
        q_y(piece).start()
        turned(wqs, piece, y, None, write(q_view(piece)))

    def pass_y(piece):
        kv_y(piece).wait_recv()
        kv_z(6 + piece).start()
        dup(6 + piece).start()

    def pass_z(n):
        kv_z(n).wait_recv()
        dup(12 + n).start()

    columns = pl.ds(pl.multiple_of(c * (D // 2), 128), D // 2)
    wg = Gather(lambda i, device: wo.at[pl.ds(pl.multiple_of(lax.div(device, 2) * 256 + i * 128, 128), 128), columns],
                ((X, Y, Z), (Y, Z, X)), me, wg_s, wg_r)

    def wdup(i, s):
        view = wg.landed(i, s)
        return remote(view, view, wd_s.at[7 * i + s], wd_r.at[7 * i + s], mate)

    def wo_in(i, s, *onward):
        wg.copy(i, s).wait_recv()
        for t in onward:
            wg.copy(i, t).start()
        wdup(i, s).start()

    SUM, TOP, LANES = pl.ds(0, HEAD), pl.ds(HEAD, HALF), pl.ds(HEAD + HALF, HALF)
    state[:, :HEAD] = jnp.zeros((4 * TOK, HEAD), jnp.float32)
    state[:, TOP] = jnp.full((4 * TOK, HALF), NEG, jnp.float32)
    state[:, LANES] = jnp.zeros((4 * TOK, HALF), jnp.float32)
    e = HEAD**-0.5 * LOG2E

    def queries(slot, first, n):
        return pl.ds(pl.multiple_of(slot * TOK + first, STRIP), n)

    def scores(at, keys):
        return dot(qbuf[at, :], kv2[0, keys, :], 1, 1)

    def weigh(at, s):
        tiles = s.shape[1] // HALF
        old = state[at, TOP]
        top = jnp.maximum(old, s.max(axis=1, keepdims=True))
        state[at, TOP] = top
        p = jnp.exp2((s - jnp.tile(top, (1, tiles))) * e)
        keep = jnp.exp2((old - top) * e)
        part = p[:, :HALF]
        for t in range(1, tiles):
            part = part + p[:, t * HALF : (t + 1) * HALF]
        state[at, LANES] = state[at, LANES] * keep + part
        return p.astype(jnp.bfloat16), keep

    def add(at, keys, p, keep):
        state[at, SUM] = state[at, SUM] * jnp.tile(keep, (1, 2)) + dot(p, kv2[1, keys, :], 1, 0)

    def whole(slot, j):
        keys = pl.ds(pl.multiple_of(j * TOK, TOK), TOK)
        ats = [queries(slot, n, STRIP) for n in range(0, TOK, STRIP)]
        s = [scores(at, keys) for at in ats]
        w = [weigh(at, t) for at, t in zip(ats, s)]
        for at, t in zip(ats, w):
            add(at, keys, *t)

    def diagonal(slot):
        keys = [pl.ds(pl.multiple_of((2 * slot + z) * TOK, TOK), n) for n in (OWN, TOK)]
        ats = [queries(slot, n, OWN) for n in (0, OWN)]
        s = [scores(at, k) for at, k in zip(ats, keys)]
        for n in range(2):
            row = n * OWN + lax.broadcasted_iota(jnp.int32, s[n].shape, 0)
            s[n] = jnp.where(row >= lax.broadcasted_iota(jnp.int32, s[n].shape, 1), s[n], HIDDEN)
        w = [weigh(at, t) for at, t in zip(ats, s)]
        for at, k, t in zip(ats, keys, w):
            add(at, k, *t)

    head = pl.ds(pl.multiple_of((2 * (2 * x + y) + c) * HEAD, HEAD), HEAD)

    def place(i):
        fx, fy = lax.div(3 - i, 2), lax.rem(3 - i, 2)
        return x + fx * (1 - 2 * x), y + fy * (1 - 2 * y)

    def out(i, core):
        x2, y2 = place(i)
        to = c if core == 0 else 1 - c
        src = qbuf.at[pl.ds(pl.multiple_of((2 * x2 + y2) * TOK + to * OWN, OWN), OWN)]
        return src, 8 * x2 + 4 * y2 + 2 * z + to, 2 * i + core

    def out_far(i, core):
        src, device, n = out(i, core)
        return remote(src, seen.at[:, head], out_s.at[n], out_r.at[n], device)

    def out_here():
        src, _, _ = out(3, 0)
        return pltpu.make_async_copy(src, seen.at[:, head], local.at[5])

    def slot_of(i):
        x2, y2 = place(i)
        return 2 * x2 + y2

    def near(i):
        slot = slot_of(i)
        lax.fori_loop(4 * x, 2 * slot + z, lambda j, _: whole(slot, j), None)
        diagonal(slot)

    def finish(i):
        slot = slot_of(i)

        def scaled(r, _):
            at = queries(slot, r * STRIP, STRIP)
            total = state[at, LANES].sum(axis=1, keepdims=True)
            qbuf[at, :] = (state[at, SUM] * (1 / total)).astype(jnp.bfloat16)

        lax.fori_loop(0, TOK // STRIP, scaled, None)
        if isinstance(i, int) and i == 3:
            out_here().start()
        else:
            out_far(i, 0).start()
        out_far(i, 1).start()

    kvg.arrived((1, 2))
    a_mate(0).wait_recv()
    a_mate(1).wait_recv()
    project_kv(0)
    project_kv(1)
    qg.arrived((0,))
    qg.start((2,))
    a_x(0).wait_recv()
    a_pass(0).start()
    pass_y(0)
    qg.arrived((1, 2))
    project_q(0)
    project_q(1)
    pass_y(1)
    project_kv(2)
    a_pass(0).wait_recv()
    project_kv(3)
    keep_w.wait()
    pair_w.wait_recv()
    wg.copy(1, 0).start()
    wg.copy(1, 1).start()
    project_q(2)
    project_q(3)
    wg.copy(0, 0).start()
    wg.copy(1, 3).start()
    for n in range(12):
        if n % 6 < 2:
            pass_z(n)
    for n in range(24):
        if n % 6 < 2:
            dup(n).wait_recv()
    near(3)
    a_x(1).wait_recv()
    a_pass(1).start()
    project_kv(4)
    a_pass(1).wait_recv()
    project_kv(5)
    pass_y(2)
    pass_y(3)
    project_q(4)
    project_q(5)
    wo_in(1, 0, 4)
    q_y(0).wait_recv()
    q_y(1).wait_recv()
    near(2)
    pass_y(4)
    pass_y(5)
    wg.copy(1, 2).start()
    wg.copy(0, 1).start()
    wg.copy(0, 3).start()
    wo_in(1, 1, 5)
    wo_in(0, 0, 2, 4)
    for n in (2, 3, 8, 9, 4, 5, 10, 11):
        pass_z(n)
    for piece in range(2, 6):
        q_y(piece).wait_recv()
    for n in range(24):
        if n % 6 > 1:
            dup(n).wait_recv()

    polls = ((2, ((1, 2, 6),)), (6, ((0, 1, 5),)), (9, ((0, 2, 6),)))

    def poll(what):
        for args in what:
            wo_in(*args)

    def step(slot, count):
        def body(j, _):
            whole(slot, j)
            for when, what in polls:
                pl.when(count + j == when)(lambda what=what: poll(what))
        return body

    def far(i, count):
        slot = slot_of(i)
        last = 2 * slot + z
        lax.fori_loop(0, last, step(slot, count), None)
        diagonal(slot)
        finish(i)

        @pl.when((x == 0) & (i == 0))
        def _():
            finish(2)
            finish(3)

        return count + last

    def rest(i, count):
        slot = slot_of(i)
        lax.fori_loop(0, 4, step(slot, count), None)
        return count + 4

    count = lax.fori_loop(0, 2, far, jnp.int32(0))

    @pl.when(x == 1)
    def _():
        rest(2, count)
        finish(2)
        rest(3, count + 4)
        finish(3)

    for i in range(2):
        wo_in(i, 3)
        wo_in(i, 4)
    def share(i, n):
        at = pl.ds(pl.multiple_of(slot_of(i) * OWN, OWN), OWN)
        return dot(seen[:, at], wo[at, pl.ds(pl.multiple_of(n * OWN, OWN), OWN)], 1, 0)

    def tile(n):
        return pl.ds(pl.multiple_of(n * OWN, OWN), OWN)

    def came(i):
        for core in range(2):
            if i < 3 or core:
                out_far(i, core).wait_recv()

    def rows_came(over_x, over_y):
        for i in range(2):
            for s, (link, path) in enumerate(SENDS):
                bits = [wg.orders[i][k] for k in (link, *path)]
                if (X in bits) == over_x and (Y in bits) == over_y:
                    wdup(i, s).wait_recv()

    def begin(n, _):
        state[tile(n), :] = share(3, n)

    def more(n, _):
        state[tile(n), :] += share(2, n)

    rows_came(False, False)
    out_here().wait()
    came(3)
    lax.fori_loop(0, D // OWN, begin, None)
    wo_in(0, 5)
    wo_in(1, 5)
    rows_came(False, True)
    came(2)
    lax.fori_loop(0, D // OWN, more, None)
    wo_in(0, 6)
    wo_in(1, 6)
    rows_came(True, False)
    rows_came(True, True)
    came(0)
    came(1)
    for n in range(D // OWN):
        cols = tile(n)
        xin[:, cols] = (xin[:, cols].astype(jnp.float32) + (state[cols, :] + share(0, n) + share(1, n))).astype(jnp.bfloat16)

    for rel in (1, 2, 3):
        kv_first(rel, wk_ref).wait_send()
        for j in range(2):
            q_first(rel, j).wait_send()
    kvg.sent()
    qg.sent()
    for h in range(2):
        a_mate(h).wait_send()
        a_x(h).wait_send()
        a_pass(h).wait_send()
    for piece in range(6):
        kv_y(piece).wait_send()
        q_y(piece).wait_send()
    for n in range(12):
        kv_z(n).wait_send()
    for n in range(24):
        dup(n).wait_send()
    pair_w.wait_send()
    wg.sent()
    for s in range(7):
        for i in range(2):
            wdup(i, s).wait_send()
    for i in range(4):
        for core in range(2):
            if i < 3 or core:
                out_far(i, core).wait_send()


def layer(x, gain, freq, wq, wk, wv, wo):
    bf, f32 = jnp.bfloat16, jnp.float32
    hbm, vmem = pl.BlockSpec(memory_space=HBM), pl.BlockSpec(memory_space=pltpu.VMEM)
    buffers = ((4, OWN, D), (D, OWN), (D, OWN), (2, 8 * TOK, HEAD), (4 * OWN, HEAD), (4 * TOK, HEAD), (4 * OWN, HEAD), (4 * OWN, D),
               (OWN, 4 * OWN))
    return pl.pallas_call(
        _layer,
        in_specs=[hbm, vmem, vmem, hbm, hbm, hbm, hbm],
        out_specs=vmem,
        out_shape=jax.ShapeDtypeStruct((OWN, D), bf),
        scratch_shapes=[
            *[pltpu.VMEM(shape, bf) for shape in buffers],
            pltpu.VMEM((4, OWN, HALF), f32), pltpu.VMEM((4, OWN, HALF), f32), pltpu.VMEM((4 * TOK, 2 * HEAD), f32),
            pltpu.SemaphoreType.DMA((SEMS,)),
        ],
        compiler_params=pltpu.CompilerParams(collective_id=0, has_side_effects=True, vmem_limit_bytes=VMEM),
        cost_estimate=pl.CostEstimate(flops=2**36, transcendentals=2**24, bytes_accessed=2**24),
    )(x, gain, freq, wq, wk, wv, wo)


def solution(mesh):
    def step(x, gain, wq, wk, wv, wo):
        freq = (THETA ** (-jnp.arange(HALF, dtype=jnp.float32) / HALF)).reshape(1, HALF)
        return layer(x, gain, freq, wq, wk, wv, wo)

    tokens, whole = P(("dp", "sp"), None), P("sp", None)
    return jax.shard_map(
        step,
        mesh=mesh,
        in_specs=(tokens, P(None), whole, whole, whole, whole),
        out_specs=tokens,
        check_vma=False,
    )
```

```python
import jax
import jax.numpy as jnp
from jax import lax
from jax.experimental import pallas as pl
from jax.experimental.pallas import tpu as pltpu
from jax.sharding import PartitionSpec as P

HEAD = 256
HALF = HEAD // 2
THETA = 10000
D = 2560
OWN = 512
TOK = 1024
NEG = -1e30
HIDDEN = 2 * NEG
LOG2E = 1.4426950408889634
LOCAL = 16
SEMS = LOCAL + 2 * (9 + 6 + 6 + 2 + 4 + 6 + 6 + 12 + 24 + 1 + 14 + 14 + 8)
STRIP = 256
VMEM = 67043328
MESH = pl.DeviceIdType.MESH
HBM = pltpu.HBM
X, Y, Z, C = 8, 4, 2, 1
ROWS = D // 16
SENDS = ((0, ()), (1, ()), (1, (0,)), (2, ()), (2, (0,)), (2, (1,)), (2, (0, 1)))
PIECES = (*((0, core, 0, OWN) for core in (0, 1)), *((1, core, first, STRIP) for first in (0, STRIP) for core in (0, 1)))


def flip(v, *bits):
    out = v
    for w in bits:
        out = out + w * (1 - 2 * lax.rem(lax.div(v, w), 2))
    return out


def remote(src, dst, send, recv, device):
    return pltpu.make_async_remote_copy(src_ref=src, dst_ref=dst, send_sem=send, recv_sem=recv, device_id={"sp": device}, device_id_type=MESH)


def dot(a, b, ca, cb):
    return lax.dot_general(a, b, (((ca,), (cb,)), ((), ())), preferred_element_type=jnp.float32)


class Gather:
    def __init__(self, view, orders, me, send_sem, recv_sem):
        self.view, self.orders, self.me, self.send_sem, self.recv_sem = view, orders, me, send_sem, recv_sem
        self.n = 2 ** len(orders[0]) - 1
        self.parts = range(len(orders))

    def copy(self, i, s):
        order = self.orders[i]
        link, path = SENDS[s]
        view = self.view(i, flip(self.me, *[order[k] for k in path]))
        return remote(view, view, self.send_sem.at[self.n * i + s], self.recv_sem.at[self.n * i + s], flip(self.me, order[link]))

    def landed(self, i, s):
        order = self.orders[i]
        link, path = SENDS[s]
        return self.view(i, flip(self.me, order[link], *[order[k] for k in path]))

    def start(self, sends, parts=None):
        for s in sends:
            for i in self.parts if parts is None else parts:
                self.copy(i, s).start()

    def arrived(self, sends, parts=None):
        for s in sends:
            for i in self.parts if parts is None else parts:
                self.copy(i, s).wait_recv()

    def sent(self):
        for i in self.parts:
            for s in range(self.n):
                self.copy(i, s).wait_send()


def _layer(x_ref, gain_ref, freq_ref, wq_ref, wk_ref, wv_ref, wo_ref, xin,
           a, wkv, wqs, kv2, kvy, qbuf, qy, wo, seen, cos_s, sin_s, state, sems):
    used = [0]

    def take(n):
        first = used[0]
        used[0] += n
        return sems.at[pl.ds(first, n)]

    local = take(LOCAL)
    wi_s, wi_r, kvg_s, kvg_r, qg_s, qg_r, ax_s, ax_r, am_s, am_r = (take(n) for n in (9, 6, 6, 2, 4) for _ in range(2))
    ky_s, ky_r, qy_s, qy_r, kz_s, kz_r, dup_s, dup_r = (take(n) for n in (6, 6, 12, 24) for _ in range(2))
    wp_s, wp_r, wg_s, wg_r, wd_s, wd_r, out_s, out_r = (take(n) for n in (1, 14, 14, 8) for _ in range(2))
    me = lax.axis_index("sp")
    c, z, y, x = (lax.rem(lax.div(me, w), 2) for w in (C, Z, Y, X))
    mate = flip(me, C)
    own_rows = pl.ds(pl.multiple_of(me * ROWS, 32), ROWS)

    barrier = pltpu.get_barrier_semaphore()
    for mask in range(1, 16):
        pl.semaphore_signal(barrier, inc=1, device_id={"sp": flip(me, *[w for w in (C, Z, Y, X) if mask & w])}, device_id_type=MESH)
    load_x = pltpu.make_async_copy(x_ref, xin, local.at[0])
    load_x.start()
    pl.semaphore_wait(barrier, 15)

    TO = ((), (C,), (X,), (X, C))

    def kv_first(rel, src):
        target = flip(me, *TO[rel])
        cols = pl.ds(pl.multiple_of(lax.div(target, 8) * 512, 512), 512)
        if rel == 0:
            return pltpu.make_async_copy(src.at[:, cols], wkv.at[own_rows], local.at[1])
        return remote(src.at[:, cols], wkv.at[own_rows], wi_s.at[rel - 1], wi_r.at[rel - 1], target)

    def q_first(rel, j):
        target = flip(me, *TO[rel])
        head = 4 * lax.div(target, 8) + 2 * j + lax.rem(target, 2)
        cols = pl.ds(pl.multiple_of(head * HEAD, HEAD), HEAD)
        dst = wqs.at[own_rows, pl.ds(j * HEAD, HEAD)]
        if rel == 0:
            return pltpu.make_async_copy(wq_ref.at[:, cols], dst, local.at[2 + j])
        n = 3 + 2 * (rel - 1) + j
        return remote(wq_ref.at[:, cols], dst, wi_s.at[n], wi_r.at[n], target)

    @pl.when(c == 0)
    def _():
        for rel, src in ((1, wv_ref), (0, wk_ref), (2, wk_ref), (3, wv_ref)):
            kv_first(rel, src).start()

    @pl.when(c == 1)
    def _():
        for rel, src in ((1, wk_ref), (0, wv_ref), (2, wv_ref), (3, wk_ref)):
            kv_first(rel, src).start()

    for rel in (1, 0, 2, 3):
        for j in range(2):
            q_first(rel, j).start()

    def rows_of(buf):
        def view(i, device):
            chip = lax.div(flip(device, X) if i else device, 2)
            return buf.at[pl.ds(pl.multiple_of(chip * (2 * ROWS), 64), 2 * ROWS)]
        return view

    kvg = Gather(rows_of(wkv), ((Y, Z), (Z, Y)), me, kvg_s, kvg_r)
    qg = Gather(rows_of(wqs), ((Y, Z), (Z, Y)), me, qg_s, qg_r)

    def quarter(fx, fc):
        return 2 * lax.div(flip(me, *([X] if fx else [])), 8) + lax.rem(flip(me, *([C] if fc else [])), 2)

    mine = quarter(0, 0)

    def a_view(h):
        return a.at[mine, pl.ds(h * 256, 256)]

    def a_mate(h):
        return remote(a_view(h), a_view(h), am_s.at[h], am_r.at[h], mate)

    def a_x(h):
        return remote(a_view(h), a_view(h), ax_s.at[h], ax_r.at[h], flip(me, X))

    def a_pass(h):
        view = a.at[quarter(1, 0), pl.ds(h * 256, 256)]
        return remote(view, view, am_s.at[2 + h], am_r.at[2 + h], mate)

    gain = gain_ref[...].astype(jnp.float32).reshape(1, D)

    def norm(r, _):
        here = pl.ds(pl.multiple_of(r * 64, 64), 64)
        wide = xin[here, :].astype(jnp.float32)
        scale = lax.rsqrt(jnp.mean(wide * wide, -1, keepdims=True) + 1e-6)
        a[mine, here, :] = (wide * scale * gain).astype(jnp.bfloat16)

    kv_first(0, wk_ref).wait()
    kv_first(1, wk_ref).wait_recv()
    kvg.start((0, 1), (0,))
    load_x.wait()
    for h in range(2):
        lax.fori_loop(4 * h, 4 * h + 4, norm, None)
        a_x(h).start()
        a_mate(h).start()
    kv_first(2, wk_ref).wait_recv()
    kv_first(3, wk_ref).wait_recv()
    kvg.start((0, 1), (1,))
    for j in range(2):
        q_first(0, j).wait()
        q_first(1, j).wait_recv()
    kvg.arrived((0,), (0,))
    kvg.start((2,), (0,))
    kvg.arrived((0,), (1,))
    kvg.start((2,), (1,))
    qg.start((0, 1), (0,))
    for j in range(2):
        q_first(2, j).wait_recv()
        q_first(3, j).wait_recv()
    qg.start((0, 1), (1,))
    wown = pl.ds(pl.multiple_of(me * 128, 128), 128)
    keep_w = pltpu.make_async_copy(wo_ref, wo.at[wown], local.at[4])
    pair_w = remote(wo_ref, wo.at[wown], wp_s.at[0], wp_r.at[0], mate)
    keep_w.start()
    pair_w.start()

    for fx in range(2):
        for fc in range(2):
            n = quarter(fx, fc)
            token = 512 * flip(me, *([X] if fx else []), *([C] if fc else []))

            def angles(r, _):
                here = pl.ds(pl.multiple_of(r * 64, 64), 64)
                place = (token + r * 64 + lax.broadcasted_iota(jnp.int32, (64, HALF), 0)).astype(jnp.float32)
                angle = place * freq_ref[...]
                cos_s[n, here, :] = jnp.cos(angle)
                sin_s[n, here, :] = jnp.sin(angle)

            lax.fori_loop(0, 8, angles, None)

    def turned(w, piece, head, plain, out):
        fx, fc, first, n = PIECES[piece]
        t4 = quarter(fx, fc)
        cols = pl.ds(pl.multiple_of(head * HEAD, HEAD), HEAD)

        def body(r, _):
            here = pl.ds(pl.multiple_of(first + r * 256, 256), 256)
            t = dot(a[t4, here, :], w[:, cols], 1, 0).astype(jnp.bfloat16).astype(jnp.float32)
            cos, sin = cos_s[t4, here, :], sin_s[t4, here, :]
            if plain is not None:
                cos, sin = jnp.where(plain == 1, 1.0, cos), jnp.where(plain == 1, 0.0, sin)
            p, q = t[:, : HALF], t[:, HALF :]
            out(r, (p * cos - q * sin).astype(jnp.bfloat16), (q * cos + p * sin).astype(jnp.bfloat16))

        lax.fori_loop(0, n // 256, body, None)

    def token_rows(piece, *bits):
        fx, fc, first, n = PIECES[piece]
        device = flip(me, *([X] if fx else []), *([C] if fc else []), *bits)
        return pl.ds(pl.multiple_of(device * OWN + first, 256), n)

    def kv_view(piece, *bits):
        return kv2.at[c, token_rows(piece, *bits)]

    def stage(buf, piece):
        fx, fc, first, n = PIECES[piece]
        return buf.at[pl.ds(pl.multiple_of(quarter(fx, fc) * OWN + first, 256), n)]

    def q_view(piece, *bits):
        fx, fc, first, n = PIECES[piece]
        device = flip(me, *([X] if fx else []), *([C] if fc else []), *bits)
        slot = 4 * lax.div(device, 8) + 2 * lax.rem(lax.div(device, 4), 2) + lax.rem(device, 2)
        return qbuf.at[pl.ds(pl.multiple_of(slot * OWN + first, 256), n)]

    def write(view):
        def out(r, left, right):
            view[pl.ds(pl.multiple_of(r * 256, 256), 256), : HALF] = left
            view[pl.ds(pl.multiple_of(r * 256, 256), 256), HALF :] = right
        return out

    def kv_y(piece):
        return remote(stage(kvy, piece), kv_view(piece), ky_s.at[piece], ky_r.at[piece], flip(me, Y))

    def q_y(piece):
        return remote(stage(qy, piece), q_view(piece), qy_s.at[piece], qy_r.at[piece], flip(me, Y))

    def kv_z(n):
        view = kv_view(n % 6, *([Y] if n >= 6 else []))
        return remote(view, view, kz_s.at[n], kz_r.at[n], flip(me, Z))

    def dup(n):
        view = kv_view(n % 6, *([Y] if n % 12 >= 6 else []), *([Z] if n >= 12 else []))
        return remote(view, view, dup_s.at[n], dup_r.at[n], mate)

    def project_kv(piece):
        turned(wkv, piece, 1 - y, c, write(stage(kvy, piece)))
        kv_y(piece).start()
        turned(wkv, piece, y, c, write(kv_view(piece)))
        kv_z(piece).start()
        dup(piece).start()

    def project_q(piece):
        turned(wqs, piece, 1 - y, None, write(stage(qy, piece)))
        q_y(piece).start()
        turned(wqs, piece, y, None, write(q_view(piece)))

    def pass_y(piece):
        kv_y(piece).wait_recv()
        kv_z(6 + piece).start()
        dup(6 + piece).start()

    def pass_z(n):
        kv_z(n).wait_recv()
        dup(12 + n).start()

    columns = pl.ds(pl.multiple_of(c * (D // 2), 128), D // 2)
    wg = Gather(lambda i, device: wo.at[pl.ds(pl.multiple_of(lax.div(device, 2) * 256 + i * 128, 128), 128), columns],
                ((X, Y, Z), (Y, Z, X)), me, wg_s, wg_r)

    def wdup(i, s):
        view = wg.landed(i, s)
        return remote(view, view, wd_s.at[7 * i + s], wd_r.at[7 * i + s], mate)

    def wo_in(i, s, *onward):
        wg.copy(i, s).wait_recv()
        for t in onward:
            wg.copy(i, t).start()
        wdup(i, s).start()

    SUM, TOP, LANES = pl.ds(0, HEAD), pl.ds(HEAD, HALF), pl.ds(HEAD + HALF, HALF)
    state[:, :HEAD] = jnp.zeros((4 * TOK, HEAD), jnp.float32)
    state[:, TOP] = jnp.full((4 * TOK, HALF), NEG, jnp.float32)
    state[:, LANES] = jnp.zeros((4 * TOK, HALF), jnp.float32)
    e = HEAD**-0.5 * LOG2E

    def queries(slot, first, n):
        return pl.ds(pl.multiple_of(slot * TOK + first, STRIP), n)

    def scores(at, keys):
        return dot(qbuf[at, :], kv2[0, keys, :], 1, 1)

    def weigh(at, s):
        tiles = s.shape[1] // HALF
        old = state[at, TOP]
        top = jnp.maximum(old, s.max(axis=1, keepdims=True))
        state[at, TOP] = top
        p = jnp.exp2((s - jnp.tile(top, (1, tiles))) * e)
        keep = jnp.exp2((old - top) * e)
        part = p[:, :HALF]
        for t in range(1, tiles):
            part = part + p[:, t * HALF : (t + 1) * HALF]
        state[at, LANES] = state[at, LANES] * keep + part
        return p.astype(jnp.bfloat16), keep

    def add(at, keys, p, keep):
        state[at, SUM] = state[at, SUM] * jnp.tile(keep, (1, 2)) + dot(p, kv2[1, keys, :], 1, 0)

    def whole(slot, j):
        keys = pl.ds(pl.multiple_of(j * TOK, TOK), TOK)
        ats = [queries(slot, n, STRIP) for n in range(0, TOK, STRIP)]
        s = [scores(at, keys) for at in ats]
        w = [weigh(at, t) for at, t in zip(ats, s)]
        for at, t in zip(ats, w):
            add(at, keys, *t)

    def diagonal(slot):
        keys = [pl.ds(pl.multiple_of((2 * slot + z) * TOK, TOK), n) for n in (OWN, TOK)]
        ats = [queries(slot, n, OWN) for n in (0, OWN)]
        s = [scores(at, k) for at, k in zip(ats, keys)]
        for n in range(2):
            row = n * OWN + lax.broadcasted_iota(jnp.int32, s[n].shape, 0)
            s[n] = jnp.where(row >= lax.broadcasted_iota(jnp.int32, s[n].shape, 1), s[n], HIDDEN)
        w = [weigh(at, t) for at, t in zip(ats, s)]
        for at, k, t in zip(ats, keys, w):
            add(at, k, *t)

    head = pl.ds(pl.multiple_of((2 * (2 * x + y) + c) * HEAD, HEAD), HEAD)

    def place(i):
        fx, fy = lax.div(3 - i, 2), lax.rem(3 - i, 2)
        return x + fx * (1 - 2 * x), y + fy * (1 - 2 * y)

    def out(i, core):
        x2, y2 = place(i)
        to = c if core == 0 else 1 - c
        src = qbuf.at[pl.ds(pl.multiple_of((2 * x2 + y2) * TOK + to * OWN, OWN), OWN)]
        return src, 8 * x2 + 4 * y2 + 2 * z + to, 2 * i + core

    def out_far(i, core):
        src, device, n = out(i, core)
        return remote(src, seen.at[:, head], out_s.at[n], out_r.at[n], device)

    def out_here():
        src, _, _ = out(3, 0)
        return pltpu.make_async_copy(src, seen.at[:, head], local.at[5])

    def slot_of(i):
        x2, y2 = place(i)
        return 2 * x2 + y2

    def near(i):
        slot = slot_of(i)
        lax.fori_loop(4 * x, 2 * slot + z, lambda j, _: whole(slot, j), None)
        diagonal(slot)

    def finish(i):
        slot = slot_of(i)

        def scaled(r, _):
            at = queries(slot, r * STRIP, STRIP)
            total = state[at, LANES].sum(axis=1, keepdims=True)
            qbuf[at, :] = (state[at, SUM] * (1 / total)).astype(jnp.bfloat16)

        lax.fori_loop(0, TOK // STRIP, scaled, None)
        pl.when(i == 3)(lambda: out_here().start())
        pl.when(i < 3)(lambda: out_far(i, 0).start())
        out_far(i, 1).start()

    kvg.arrived((1, 2))
    a_mate(0).wait_recv()
    a_mate(1).wait_recv()
    project_kv(0)
    project_kv(1)
    qg.arrived((0,))
    qg.start((2,))
    a_x(0).wait_recv()
    a_pass(0).start()
    pass_y(0)
    qg.arrived((1, 2))
    project_q(0)
    project_q(1)
    pass_y(1)
    project_kv(2)
    a_pass(0).wait_recv()
    project_kv(3)
    keep_w.wait()
    pair_w.wait_recv()
    wg.copy(1, 0).start()
    wg.copy(1, 1).start()
    project_q(2)
    project_q(3)
    wg.copy(0, 0).start()
    wg.copy(1, 3).start()
    for n in range(12):
        if n % 6 < 2:
            pass_z(n)
    for n in range(24):
        if n % 6 < 2:
            dup(n).wait_recv()
    near(3)
    a_x(1).wait_recv()
    a_pass(1).start()
    project_kv(4)
    a_pass(1).wait_recv()
    project_kv(5)
    pass_y(2)
    pass_y(3)
    project_q(4)
    project_q(5)
    wo_in(1, 0, 4)
    q_y(0).wait_recv()
    q_y(1).wait_recv()
    near(2)
    pass_y(4)
    pass_y(5)
    wg.copy(1, 2).start()
    wg.copy(0, 1).start()
    wg.copy(0, 3).start()
    wo_in(1, 1, 5)
    wo_in(0, 0, 2, 4)
    for n in (2, 3, 8, 9, 4, 5):
        pass_z(n)

    @pl.when(x == 0)
    def _():
        lax.fori_loop(0, 4, lambda j, _: whole(slot_of(1), j), None)

    for n in (10, 11):
        pass_z(n)
    for piece in range(2, 6):
        q_y(piece).wait_recv()
    for n in range(24):
        if n % 6 > 1:
            dup(n).wait_recv()

    def poll_a():
        wo_in(1, 2, 6)

    def poll_b():
        wo_in(0, 1, 5)

    def poll_c():
        wo_in(0, 2, 6)

    def far(i, _):
        slot = slot_of(i)

        def body(j, _):
            whole(slot, j)
            pl.when((x == 0) & (i == 0) & (j == 2))(poll_b)

        lax.fori_loop(4 * (1 - x) * i, 2 * slot + z, body, None)
        diagonal(slot)
        finish(i)

        @pl.when((x == 0) & (i == 1))
        def _():
            poll_a()
            lax.fori_loop(2, 4, lambda n, _: finish(n), None)

        pl.when((x == 0) & (i == 0))(poll_c)
        pl.when((x == 1) & (i == 1))(poll_b)

    def rest(i, _):
        slot = slot_of(i)

        def body(j, _):
            whole(slot, j)
            pl.when((i == 2) & (j == 1))(poll_a)
            pl.when((i == 3) & (j == 1))(poll_c)

        lax.fori_loop(0, 4, body, None)
        finish(i)

    def turn(n, _):
        pl.when((n == 0) | (n == 3))(lambda: rest(2 + lax.div(n, 3), None))
        pl.when((n == 1) | (n == 2))(lambda: far(2 - n, None))

    lax.fori_loop(1 - x, 3 + x, turn, None)
    for s in (3, 4):
        for i in range(2):
            wo_in(i, s)
    def share(i, n):
        at = pl.ds(pl.multiple_of(slot_of(i) * OWN, OWN), OWN)
        return dot(seen[:, at], wo[at, pl.ds(pl.multiple_of(n * OWN, OWN), OWN)], 1, 0)

    def tile(n):
        return pl.ds(pl.multiple_of(n * OWN, OWN), OWN)

    def came(i):
        for core in range(2):
            if i < 3 or core:
                out_far(i, core).wait_recv()

    def rows_came(over_x, over_y):
        for i in range(2):
            for s, (link, path) in enumerate(SENDS):
                bits = [wg.orders[i][k] for k in (link, *path)]
                if (X in bits) == over_x and (Y in bits) == over_y:
                    wdup(i, s).wait_recv()

    def begin(n, _):
        state[tile(n), :] = share(3, n)

    rows_came(False, False)
    out_here().wait()
    came(3)
    lax.fori_loop(0, D // OWN, begin, None)
    for s in (5, 6):
        for i in range(2):
            wo_in(i, s)
    rows_came(False, True)
    rows_came(True, False)
    came(2)
    came(1)

    def more(n, _):
        state[tile(n), :] += share(1, n) + share(2, n)

    lax.fori_loop(0, D // OWN, more, None)
    rows_came(True, True)
    came(0)
    for n in range(D // OWN):
        cols = tile(n)
        xin[:, cols] = (xin[:, cols].astype(jnp.float32) + (state[cols, :] + share(0, n))).astype(jnp.bfloat16)

    for rel in (1, 2, 3):
        kv_first(rel, wk_ref).wait_send()
        for j in range(2):
            q_first(rel, j).wait_send()
    kvg.sent()
    qg.sent()
    for h in range(2):
        a_mate(h).wait_send()
        a_x(h).wait_send()
        a_pass(h).wait_send()
    for piece in range(6):
        kv_y(piece).wait_send()
        q_y(piece).wait_send()
    for n in range(12):
        kv_z(n).wait_send()
    for n in range(24):
        dup(n).wait_send()
    pair_w.wait_send()
    wg.sent()
    for s in range(7):
        for i in range(2):
            wdup(i, s).wait_send()
    for i in range(4):
        for core in range(2):
            if i < 3 or core:
                out_far(i, core).wait_send()


def layer(x, gain, freq, wq, wk, wv, wo):
    bf, f32 = jnp.bfloat16, jnp.float32
    hbm, vmem = pl.BlockSpec(memory_space=HBM), pl.BlockSpec(memory_space=pltpu.VMEM)
    buffers = ((4, OWN, D), (D, OWN), (D, OWN), (2, 8 * TOK, HEAD), (4 * OWN, HEAD), (4 * TOK, HEAD), (4 * OWN, HEAD), (4 * OWN, D),
               (OWN, 4 * OWN))
    return pl.pallas_call(
        _layer,
        in_specs=[hbm, vmem, vmem, hbm, hbm, hbm, hbm],
        out_specs=vmem,
        out_shape=jax.ShapeDtypeStruct((OWN, D), bf),
        scratch_shapes=[
            *[pltpu.VMEM(shape, bf) for shape in buffers],
            pltpu.VMEM((4, OWN, HALF), f32), pltpu.VMEM((4, OWN, HALF), f32), pltpu.VMEM((4 * TOK, 2 * HEAD), f32),
            pltpu.SemaphoreType.DMA((SEMS,)),
        ],
        compiler_params=pltpu.CompilerParams(collective_id=0, has_side_effects=True, vmem_limit_bytes=VMEM),
        cost_estimate=pl.CostEstimate(flops=2**36, transcendentals=2**24, bytes_accessed=2**24),
    )(x, gain, freq, wq, wk, wv, wo)


def solution(mesh):
    def step(x, gain, wq, wk, wv, wo):
        freq = (THETA ** (-jnp.arange(HALF, dtype=jnp.float32) / HALF)).reshape(1, HALF)
        return layer(x, gain, freq, wq, wk, wv, wo)

    tokens, whole = P(("dp", "sp"), None), P("sp", None)
    return jax.shard_map(
        step,
        mesh=mesh,
        in_specs=(tokens, P(None), whole, whole, whole, whole),
        out_specs=tokens,
        check_vma=False,
    )
```

```python
import jax
import jax.numpy as jnp
import numpy as np
from jax import lax
from jax.experimental import pallas as pl
from jax.experimental.pallas import tpu as pltpu
from jax.sharding import PartitionSpec as P

HEAD = 256
HALF = HEAD // 2
THETA = 10000
D = 2560
OWN = 512
TOK = 1024
NEG = -1e30
HIDDEN = 2 * NEG
LOG2E = 1.4426950408889634
LOCAL = 16
SEMS = LOCAL + 2 * (9 + 6 + 6 + 2 + 4 + 6 + 6 + 12 + 24 + 1 + 14 + 14 + 8)
STRIP = 256
BLOCK = 64
VMEM = 67043328
MESH = pl.DeviceIdType.MESH
HBM = pltpu.HBM
X, Y, Z, C = 8, 4, 2, 1
ROWS = D // 16
SENDS = ((0, ()), (1, ()), (1, (0,)), (2, ()), (2, (0,)), (2, (1,)), (2, (0, 1)))
PIECES = (*((0, core, 0, OWN) for core in (0, 1)), *((1, core, first, STRIP) for first in (0, STRIP) for core in (0, 1)))


def flip(v, *bits):
    out = v
    for w in bits:
        out = out + w * (1 - 2 * lax.rem(lax.div(v, w), 2))
    return out


def remote(src, dst, send, recv, device):
    return pltpu.make_async_remote_copy(src_ref=src, dst_ref=dst, send_sem=send, recv_sem=recv, device_id={"sp": device}, device_id_type=MESH)


def dot(a, b, ca, cb):
    return lax.dot_general(a, b, (((ca,), (cb,)), ((), ())), preferred_element_type=jnp.float32)


class Gather:
    def __init__(self, view, orders, me, send_sem, recv_sem):
        self.view, self.orders, self.me, self.send_sem, self.recv_sem = view, orders, me, send_sem, recv_sem
        self.n = 2 ** len(orders[0]) - 1
        self.parts = range(len(orders))

    def copy(self, i, s):
        order = self.orders[i]
        link, path = SENDS[s]
        view = self.view(i, flip(self.me, *[order[k] for k in path]))
        return remote(view, view, self.send_sem.at[self.n * i + s], self.recv_sem.at[self.n * i + s], flip(self.me, order[link]))

    def landed(self, i, s):
        order = self.orders[i]
        link, path = SENDS[s]
        return self.view(i, flip(self.me, order[link], *[order[k] for k in path]))

    def start(self, sends, parts=None):
        for s in sends:
            for i in self.parts if parts is None else parts:
                self.copy(i, s).start()

    def arrived(self, sends, parts=None):
        for s in sends:
            for i in self.parts if parts is None else parts:
                self.copy(i, s).wait_recv()

    def sent(self):
        for i in self.parts:
            for s in range(self.n):
                self.copy(i, s).wait_send()


def _layer(x_ref, gain_ref, freq_ref, wq_ref, wk_ref, wv_ref, wo_ref, y_ref,
           xin, a, wkv, wqs, kv2, kvy, qbuf, qy, wo, seen, cos_s, sin_s, state, sems):
    used = [0]

    def take(n):
        first = used[0]
        used[0] += n
        return sems.at[pl.ds(first, n)]

    local = take(LOCAL)
    wi_s, wi_r, kvg_s, kvg_r, qg_s, qg_r, ax_s, ax_r, am_s, am_r = (take(n) for n in (9, 6, 6, 2, 4) for _ in range(2))
    ky_s, ky_r, qy_s, qy_r, kz_s, kz_r, dup_s, dup_r = (take(n) for n in (6, 6, 12, 24) for _ in range(2))
    wp_s, wp_r, wg_s, wg_r, wd_s, wd_r, out_s, out_r = (take(n) for n in (1, 14, 14, 8) for _ in range(2))
    me = lax.axis_index("sp")
    c, z, y, x = (lax.rem(lax.div(me, w), 2) for w in (C, Z, Y, X))
    mate = flip(me, C)
    own_rows = pl.ds(pl.multiple_of(me * ROWS, 32), ROWS)

    barrier = pltpu.get_barrier_semaphore()
    for mask in range(1, 16):
        pl.semaphore_signal(barrier, inc=1, device_id={"sp": flip(me, *[w for w in (C, Z, Y, X) if mask & w])}, device_id_type=MESH)
    load_x = pltpu.make_async_copy(x_ref, xin, local.at[0])
    load_x.start()
    pl.semaphore_wait(barrier, 15)

    TO = ((), (C,), (X,), (X, C))

    def kv_first(rel, src):
        target = flip(me, *TO[rel])
        cols = pl.ds(pl.multiple_of(lax.div(target, 8) * 512, 512), 512)
        if rel == 0:
            return pltpu.make_async_copy(src.at[:, cols], wkv.at[own_rows], local.at[1])
        return remote(src.at[:, cols], wkv.at[own_rows], wi_s.at[rel - 1], wi_r.at[rel - 1], target)

    def q_first(rel, j):
        target = flip(me, *TO[rel])
        head = 4 * lax.div(target, 8) + 2 * j + lax.rem(target, 2)
        cols = pl.ds(pl.multiple_of(head * HEAD, HEAD), HEAD)
        dst = wqs.at[own_rows, pl.ds(j * HEAD, HEAD)]
        if rel == 0:
            return pltpu.make_async_copy(wq_ref.at[:, cols], dst, local.at[2 + j])
        n = 3 + 2 * (rel - 1) + j
        return remote(wq_ref.at[:, cols], dst, wi_s.at[n], wi_r.at[n], target)

    @pl.when(c == 0)
    def _():
        for rel, src in ((1, wv_ref), (0, wk_ref), (2, wk_ref), (3, wv_ref)):
            kv_first(rel, src).start()

    @pl.when(c == 1)
    def _():
        for rel, src in ((1, wk_ref), (0, wv_ref), (2, wv_ref), (3, wk_ref)):
            kv_first(rel, src).start()

    for rel in (1, 0, 2, 3):
        for j in range(2):
            q_first(rel, j).start()

    def rows_of(buf):
        def view(i, device):
            chip = lax.div(flip(device, X) if i else device, 2)
            return buf.at[pl.ds(pl.multiple_of(chip * (2 * ROWS), 64), 2 * ROWS)]
        return view

    kvg = Gather(rows_of(wkv), ((Y, Z), (Z, Y)), me, kvg_s, kvg_r)
    qg = Gather(rows_of(wqs), ((Y, Z), (Z, Y)), me, qg_s, qg_r)

    def quarter(fx, fc):
        return 2 * lax.div(flip(me, *([X] if fx else [])), 8) + lax.rem(flip(me, *([C] if fc else [])), 2)

    mine = quarter(0, 0)

    def a_view(h):
        return a.at[mine, pl.ds(h * 256, 256)]

    def a_mate(h):
        return remote(a_view(h), a_view(h), am_s.at[h], am_r.at[h], mate)

    def a_x(h):
        return remote(a_view(h), a_view(h), ax_s.at[h], ax_r.at[h], flip(me, X))

    def a_pass(h):
        view = a.at[quarter(1, 0), pl.ds(h * 256, 256)]
        return remote(view, view, am_s.at[2 + h], am_r.at[2 + h], mate)

    gain = gain_ref[...].astype(jnp.float32).reshape(1, D)

    def norm(r, _):
        here = pl.ds(pl.multiple_of(r * 64, 64), 64)
        wide = xin[here, :].astype(jnp.float32)
        scale = lax.rsqrt(jnp.mean(wide * wide, -1, keepdims=True) + 1e-6)
        a[mine, here, :] = (wide * scale * gain).astype(jnp.bfloat16)

    kv_first(0, wk_ref).wait()
    kv_first(1, wk_ref).wait_recv()
    kvg.start((0, 1), (0,))
    load_x.wait()
    for h in range(2):
        lax.fori_loop(4 * h, 4 * h + 4, norm, None)
        a_x(h).start()
        a_mate(h).start()
    kv_first(2, wk_ref).wait_recv()
    kv_first(3, wk_ref).wait_recv()
    kvg.start((0, 1), (1,))
    for j in range(2):
        q_first(0, j).wait()
        q_first(1, j).wait_recv()
    kvg.arrived((0,), (0,))
    kvg.start((2,), (0,))
    kvg.arrived((0,), (1,))
    kvg.start((2,), (1,))
    qg.start((0, 1), (0,))
    for j in range(2):
        q_first(2, j).wait_recv()
        q_first(3, j).wait_recv()
    qg.start((0, 1), (1,))
    wown = pl.ds(pl.multiple_of(me * 128, 128), 128)
    keep_w = pltpu.make_async_copy(wo_ref, wo.at[wown], local.at[4])
    pair_w = remote(wo_ref, wo.at[wown], wp_s.at[0], wp_r.at[0], mate)
    keep_w.start()
    pair_w.start()

    for fx in range(2):
        for fc in range(2):
            n = quarter(fx, fc)
            token = 512 * flip(me, *([X] if fx else []), *([C] if fc else []))

            def angles(r, _):
                here = pl.ds(pl.multiple_of(r * 64, 64), 64)
                place = (token + r * 64 + lax.broadcasted_iota(jnp.int32, (64, HALF), 0)).astype(jnp.float32)
                angle = place * freq_ref[...]
                cos_s[n, here, :] = jnp.cos(angle)
                sin_s[n, here, :] = jnp.sin(angle)

            lax.fori_loop(0, 8, angles, None)

    def turned(w, piece, head, plain, out):
        fx, fc, first, n = PIECES[piece]
        t4 = quarter(fx, fc)
        cols = pl.ds(pl.multiple_of(head * HEAD, HEAD), HEAD)

        def body(r, _):
            here = pl.ds(pl.multiple_of(first + r * 256, 256), 256)
            t = dot(a[t4, here, :], w[:, cols], 1, 0).astype(jnp.bfloat16).astype(jnp.float32)
            cos, sin = cos_s[t4, here, :], sin_s[t4, here, :]
            if plain is not None:
                cos, sin = jnp.where(plain == 1, 1.0, cos), jnp.where(plain == 1, 0.0, sin)
            p, q = t[:, : HALF], t[:, HALF :]
            out(r, (p * cos - q * sin).astype(jnp.bfloat16), (q * cos + p * sin).astype(jnp.bfloat16))

        lax.fori_loop(0, n // 256, body, None)

    def token_rows(piece, *bits):
        fx, fc, first, n = PIECES[piece]
        device = flip(me, *([X] if fx else []), *([C] if fc else []), *bits)
        return pl.ds(pl.multiple_of(device * OWN + first, 256), n)

    def kv_view(piece, *bits):
        return kv2.at[c, token_rows(piece, *bits)]

    def stage(buf, piece):
        fx, fc, first, n = PIECES[piece]
        return buf.at[pl.ds(pl.multiple_of(quarter(fx, fc) * OWN + first, 256), n)]

    def q_view(piece, *bits):
        fx, fc, first, n = PIECES[piece]
        device = flip(me, *([X] if fx else []), *([C] if fc else []), *bits)
        slot = 4 * lax.div(device, 8) + 2 * lax.rem(lax.div(device, 4), 2) + lax.rem(device, 2)
        return qbuf.at[pl.ds(pl.multiple_of(slot * OWN + first, 256), n)]

    def write(view):
        def out(r, left, right):
            view[pl.ds(pl.multiple_of(r * 256, 256), 256), : HALF] = left
            view[pl.ds(pl.multiple_of(r * 256, 256), 256), HALF :] = right
        return out

    def kv_y(piece):
        return remote(stage(kvy, piece), kv_view(piece), ky_s.at[piece], ky_r.at[piece], flip(me, Y))

    def q_y(piece):
        return remote(stage(qy, piece), q_view(piece), qy_s.at[piece], qy_r.at[piece], flip(me, Y))

    def kv_z(n):
        view = kv_view(n % 6, *([Y] if n >= 6 else []))
        return remote(view, view, kz_s.at[n], kz_r.at[n], flip(me, Z))

    def dup(n):
        view = kv_view(n % 6, *([Y] if n % 12 >= 6 else []), *([Z] if n >= 12 else []))
        return remote(view, view, dup_s.at[n], dup_r.at[n], mate)

    def project_kv(piece):
        turned(wkv, piece, 1 - y, c, write(stage(kvy, piece)))
        kv_y(piece).start()
        turned(wkv, piece, y, c, write(kv_view(piece)))
        kv_z(piece).start()
        dup(piece).start()

    def project_q(piece):
        turned(wqs, piece, 1 - y, None, write(stage(qy, piece)))
        q_y(piece).start()
        turned(wqs, piece, y, None, write(q_view(piece)))

    def pass_y(piece):
        kv_y(piece).wait_recv()
        kv_z(6 + piece).start()
        dup(6 + piece).start()

    def pass_z(n):
        kv_z(n).wait_recv()
        dup(12 + n).start()

    columns = pl.ds(pl.multiple_of(c * (D // 2), 128), D // 2)
    wg = Gather(lambda i, device: wo.at[pl.ds(pl.multiple_of(lax.div(device, 2) * 256 + i * 128, 128), 128), columns],
                ((X, Y, Z), (Y, Z, X)), me, wg_s, wg_r)

    def wdup(i, s):
        view = wg.landed(i, s)
        return remote(view, view, wd_s.at[7 * i + s], wd_r.at[7 * i + s], mate)

    def wo_in(i, s, *onward):
        wg.copy(i, s).wait_recv()
        for t in onward:
            wg.copy(i, t).start()
        wdup(i, s).start()

    SUM, TOP, LANES = pl.ds(0, HEAD), pl.ds(HEAD, HALF), pl.ds(HEAD + HALF, HALF)
    state[:, :HEAD] = jnp.zeros((4 * TOK, HEAD), jnp.float32)
    state[:, TOP] = jnp.full((4 * TOK, HALF), NEG, jnp.float32)
    state[:, LANES] = jnp.zeros((4 * TOK, HALF), jnp.float32)
    e = HEAD**-0.5 * LOG2E

    def queries(slot, first, n):
        return pl.ds(pl.multiple_of(slot * TOK + first, STRIP), n)

    def scores(at, keys):
        return dot(qbuf[at, :], kv2[0, keys, :], 1, 1)

    def weigh(at, s):
        tiles = s.shape[1] // HALF
        old = state[at, TOP]
        top = jnp.maximum(old, s.max(axis=1, keepdims=True))
        state[at, TOP] = top
        p = jnp.exp2((s - jnp.tile(top, (1, tiles))) * e)
        keep = jnp.exp2((old - top) * e)
        part = p[:, :HALF]
        for t in range(1, tiles):
            part = part + p[:, t * HALF : (t + 1) * HALF]
        state[at, LANES] = state[at, LANES] * keep + part
        return p.astype(jnp.bfloat16), keep

    def add(at, keys, p, keep):
        state[at, SUM] = state[at, SUM] * jnp.tile(keep, (1, 2)) + dot(p, kv2[1, keys, :], 1, 0)

    def whole(slot, j, first=0, n=TOK, hide=None):
        keys = pl.ds(pl.multiple_of(j * TOK, TOK), TOK)
        ats = [queries(slot, first + k, STRIP) for k in range(0, n, STRIP)]
        s = [scores(at, keys) for at in ats]
        if hide is not None:
            s = [hide(first + k * STRIP, t) for k, t in enumerate(s)]
        w = [weigh(at, t) for at, t in zip(ats, s)]
        for at, t in zip(ats, w):
            add(at, keys, *t)

    def later(first, s):
        row = first + lax.broadcasted_iota(jnp.int32, s.shape, 0)
        return jnp.where(row >= lax.broadcasted_iota(jnp.int32, s.shape, 1), s, HIDDEN)

    def diagonal(slot):
        keys = [pl.ds(pl.multiple_of((2 * slot + z) * TOK, TOK), n) for n in (OWN, TOK)]
        ats = [queries(slot, n, OWN) for n in (0, OWN)]
        s = [scores(at, k) for at, k in zip(ats, keys)]
        s = [later(n * OWN, t) for n, t in enumerate(s)]
        w = [weigh(at, t) for at, t in zip(ats, s)]
        for at, k, t in zip(ats, keys, w):
            add(at, k, *t)

    head = pl.ds(pl.multiple_of((2 * (2 * x + y) + c) * HEAD, HEAD), HEAD)

    def place(i):
        fx, fy = lax.div(3 - i, 2), lax.rem(3 - i, 2)
        return x + fx * (1 - 2 * x), y + fy * (1 - 2 * y)

    def out(i, core):
        x2, y2 = place(i)
        to = c if core == 0 else 1 - c
        src = qbuf.at[pl.ds(pl.multiple_of((2 * x2 + y2) * TOK + to * OWN, OWN), OWN)]
        return src, 8 * x2 + 4 * y2 + 2 * z + to, 2 * i + core

    def out_far(i, core):
        src, device, n = out(i, core)
        return remote(src, seen.at[:, head], out_s.at[n], out_r.at[n], device)

    def out_here():
        src, _, _ = out(3, 0)
        return pltpu.make_async_copy(src, seen.at[:, head], local.at[5])

    def slot_of(i):
        x2, y2 = place(i)
        return 2 * x2 + y2

    def near(i):
        slot = slot_of(i)
        lax.fori_loop(4 * x, 2 * slot + z, lambda j, _: whole(slot, j), None)
        diagonal(slot)

    def scale(slot, first, n):
        def scaled(r, _):
            at = queries(slot, first + r * STRIP, STRIP)
            total = state[at, LANES].sum(axis=1, keepdims=True)
            qbuf[at, :] = (state[at, SUM] * (1 / total)).astype(jnp.bfloat16)

        lax.fori_loop(0, n // STRIP, scaled, None)

    def finish(i):
        scale(slot_of(i), 0, TOK)
        pl.when(i == 3)(lambda: out_here().start())
        pl.when(i < 3)(lambda: out_far(i, 0).start())
        out_far(i, 1).start()

    kvg.arrived((1, 2))
    a_mate(0).wait_recv()
    a_mate(1).wait_recv()
    project_kv(0)
    project_kv(1)
    qg.arrived((0,))
    qg.start((2,))
    a_x(0).wait_recv()
    a_pass(0).start()
    pass_y(0)
    qg.arrived((1, 2))
    project_q(0)
    project_q(1)
    pass_y(1)
    project_kv(2)
    a_pass(0).wait_recv()
    project_kv(3)
    keep_w.wait()
    pair_w.wait_recv()
    wg.copy(1, 0).start()
    wg.copy(1, 1).start()
    project_q(2)
    project_q(3)
    wg.copy(0, 0).start()
    wg.copy(1, 3).start()
    for n in range(12):
        if n % 6 < 2:
            pass_z(n)
    for n in range(24):
        if n % 6 < 2:
            dup(n).wait_recv()
    near(3)
    a_x(1).wait_recv()
    a_pass(1).start()
    project_kv(4)
    a_pass(1).wait_recv()
    project_kv(5)
    pass_y(2)
    pass_y(3)
    project_q(4)
    project_q(5)
    wo_in(1, 0, 4)
    q_y(0).wait_recv()
    q_y(1).wait_recv()
    near(2)
    pass_y(4)
    pass_y(5)
    wg.copy(1, 2).start()
    wg.copy(0, 1).start()
    wg.copy(0, 3).start()
    wo_in(1, 1, 5)
    wo_in(0, 0, 2, 4)
    for n in (2, 3, 8, 9, 4, 5):
        pass_z(n)

    for n in range(2, 6):
        dup(n).wait_recv()

    def ahead(n, _):
        whole(slot_of(1 + x * (1 + n)), (1 - x) * n + x * (2 * y + z))

    lax.fori_loop(0, 4 - 2 * x, ahead, None)
    for n in (10, 11):
        pass_z(n)
    for piece in range(2, 6):
        q_y(piece).wait_recv()
    for n in range(6, 24):
        if n % 6 > 1:
            dup(n).wait_recv()

    def poll_a():
        wo_in(1, 2, 6)

    def poll_b():
        wo_in(0, 1, 5)

    def poll_c():
        wo_in(0, 2, 6)

    def far_x():
        slot = slot_of(1)
        lax.fori_loop(4 * (1 - x), 2 * slot + z, lambda j, _: whole(slot, j), None)
        diagonal(slot)
        finish(1)
        poll_a()

        @pl.when(x == 0)
        def _():
            lax.fori_loop(2, 4, lambda n, _: finish(n), None)

    def far_diagonal():
        slot = slot_of(0)
        last = 2 * slot + z

        def half(h, _):
            first = h * OWN
            lax.fori_loop(0, last, lambda j, _: whole(slot, j, first, OWN), None)
            whole(slot, last, first, OWN, later)
            scale(slot, first, OWN)
            pl.when(h == c)(lambda: out_far(0, 0).start())
            pl.when(h != c)(lambda: out_far(0, 1).start())
            pl.when((x == 0) & (h == 0))(poll_b)

        lax.fori_loop(0, 2, half, None)

        @pl.when(x == 0)
        def _():
            poll_c()
            poll_d()

    def poll_d():
        for s in (3, 4):
            for i in range(2):
                wo_in(i, s)

    def rest(i):
        slot = slot_of(i)

        def body(k, _):
            whole(slot, lax.rem(2 * y + z + k, 4))
            if i == 3:
                pl.when(k == 1)(poll_c)
                pl.when(k == 2)(poll_d)

        lax.fori_loop(1, 4, body, None)
        finish(i)
        if i == 2:
            poll_b()

    far_x()

    @pl.when(x == 1)
    def _():
        rest(2)

    far_diagonal()

    @pl.when(x == 1)
    def _():
        rest(3)

    def share(i, n):
        at = pl.ds(pl.multiple_of(slot_of(i) * OWN, OWN), OWN)
        return dot(seen[:, at], wo[at, pl.ds(pl.multiple_of(n * OWN, OWN), OWN)], 1, 0)

    def tile(n):
        return pl.ds(pl.multiple_of(n * OWN, OWN), OWN)

    def came(i):
        for core in range(2):
            if i < 3 or core:
                out_far(i, core).wait_recv()

    def rows_came(*over):
        for i in range(2):
            for s, (link, path) in enumerate(SENDS):
                bits = [wg.orders[i][k] for k in (link, *path)]
                if {X, Y}.intersection(bits) == set(over):
                    wdup(i, s).wait_recv()

    def begin(n, _):
        state[tile(n), :] = share(3, n)

    rows_came()
    out_here().wait()
    came(3)
    lax.fori_loop(0, D // OWN, begin, None)
    for i in range(2):
        wo_in(i, 5)
    rows_came(Y)
    rows_came(X)
    came(2)
    came(1)

    def more(n, _):
        state[tile(n), :] += share(1, n) + share(2, n)

    lax.fori_loop(0, D // OWN, more, None)
    for i in range(2):
        wo_in(i, 6)
    def result(n):
        return pltpu.make_async_copy(xin.at[:, tile(n)], y_ref.at[:, tile(n)], local.at[6 + n])

    rows_came(X, Y)
    came(0)
    for n in range(D // OWN):
        cols = tile(n)
        xin[:, cols] = (xin[:, cols].astype(jnp.float32) + (state[cols, :] + share(0, n))).astype(jnp.bfloat16)
        result(n).start()

    for rel in (1, 2, 3):
        kv_first(rel, wk_ref).wait_send()
        for j in range(2):
            q_first(rel, j).wait_send()
    kvg.sent()
    qg.sent()
    for h in range(2):
        a_mate(h).wait_send()
        a_x(h).wait_send()
        a_pass(h).wait_send()
    for piece in range(6):
        kv_y(piece).wait_send()
        q_y(piece).wait_send()
    for n in range(12):
        kv_z(n).wait_send()
    for n in range(24):
        dup(n).wait_send()
    pair_w.wait_send()
    wg.sent()
    for s in range(7):
        for i in range(2):
            wdup(i, s).wait_send()
    for i in range(4):
        for core in range(2):
            if i < 3 or core:
                out_far(i, core).wait_send()
    for n in range(D // OWN):
        result(n).wait()


def layer(x, gain, freq, wq, wk, wv, wo):
    bf, f32 = jnp.bfloat16, jnp.float32
    hbm, vmem = pl.BlockSpec(memory_space=HBM), pl.BlockSpec(memory_space=pltpu.VMEM)
    buffers = ((OWN, D), (4, OWN, D), (D, OWN), (D, OWN), (2, 8 * TOK, HEAD), (4 * OWN, HEAD), (4 * TOK, HEAD), (4 * OWN, HEAD), (4 * OWN, D),
               (OWN, 4 * OWN))
    return pl.pallas_call(
        _layer,
        in_specs=[hbm, vmem, vmem, hbm, hbm, hbm, hbm],
        out_specs=hbm,
        out_shape=jax.ShapeDtypeStruct((OWN, D), bf),
        scratch_shapes=[
            *[pltpu.VMEM(shape, bf) for shape in buffers],
            pltpu.VMEM((4, OWN, HALF), f32), pltpu.VMEM((4, OWN, HALF), f32), pltpu.VMEM((4 * TOK, 2 * HEAD), f32),
            pltpu.SemaphoreType.DMA((SEMS,)),
        ],
        compiler_params=pltpu.CompilerParams(collective_id=0, has_side_effects=True, vmem_limit_bytes=VMEM),
        cost_estimate=pl.CostEstimate(flops=2**36, transcendentals=2**24, bytes_accessed=2**24),
    )(x, gain, freq, wq, wk, wv, wo)


def _pass(y_ref, out_ref, buf, ins, outs):
    def part(n):
        return pl.ds(n * BLOCK, BLOCK)

    def read(n):
        return pltpu.make_async_copy(y_ref.at[part(n)], buf.at[part(n)], ins.at[n])

    def written(n):
        return pltpu.make_async_copy(buf.at[part(n)], out_ref.at[part(n)], outs.at[n])

    for n in range(OWN // BLOCK):
        read(n).start()
    for n in range(OWN // BLOCK):
        read(n).wait()
        written(n).start()
    for n in range(OWN // BLOCK):
        written(n).wait()


def passed(y):
    hbm, sems = pl.BlockSpec(memory_space=HBM), pltpu.SemaphoreType.DMA((OWN // BLOCK,))
    return pl.pallas_call(_pass, in_specs=[hbm], out_specs=hbm, out_shape=jax.ShapeDtypeStruct((OWN, D), y.dtype),
                          scratch_shapes=[pltpu.VMEM((OWN, D), y.dtype), sems, sems])(y)


def solution(mesh):
    def step(x, gain, wq, wk, wv, wo):
        freq = jnp.asarray((THETA ** (-np.arange(HALF) / HALF)).astype(np.float32).reshape(1, HALF))
        return passed(layer(x, gain, freq, wq, wk, wv, wo))

    tokens, whole = P(("dp", "sp"), None), P("sp", None)
    return jax.shard_map(
        step,
        mesh=mesh,
        in_specs=(tokens, P(None), whole, whole, whole, whole),
        out_specs=tokens,
        check_vma=False,
    )
```

```python
import jax
import jax.numpy as jnp
import numpy as np
from jax import lax
from jax.experimental import pallas as pl
from jax.experimental.pallas import tpu as pltpu
from jax.sharding import PartitionSpec as P

HEAD = 256
HALF = HEAD // 2
THETA = 10000
D = 2560
OWN = 512
TOK = 1024
NEG = -1e30
HIDDEN = 2 * NEG
LOG2E = 1.4426950408889634
LOCAL = 16
SEMS = LOCAL + 2 * (9 + 6 + 6 + 2 + 4 + 6 + 6 + 12 + 24 + 1 + 14 + 14 + 8)
STRIP = 256
BLOCK = 64
VMEM = 67043328
MESH = pl.DeviceIdType.MESH
HBM = pltpu.HBM
X, Y, Z, C = 8, 4, 2, 1
ROWS = D // 16
SENDS = ((0, ()), (1, ()), (1, (0,)), (2, ()), (2, (0,)), (2, (1,)), (2, (0, 1)))
PIECES = (*((0, core, 0, OWN) for core in (0, 1)), *((1, core, first, STRIP) for first in (0, STRIP) for core in (0, 1)))


def flip(v, *bits):
    out = v
    for w in bits:
        out = out + w * (1 - 2 * lax.rem(lax.div(v, w), 2))
    return out


def remote(src, dst, send, recv, device):
    return pltpu.make_async_remote_copy(src_ref=src, dst_ref=dst, send_sem=send, recv_sem=recv, device_id={"sp": device}, device_id_type=MESH)


def dot(a, b, ca, cb):
    return lax.dot_general(a, b, (((ca,), (cb,)), ((), ())), preferred_element_type=jnp.float32)


class Gather:
    def __init__(self, view, orders, me, send_sem, recv_sem):
        self.view, self.orders, self.me, self.send_sem, self.recv_sem = view, orders, me, send_sem, recv_sem
        self.n = 2 ** len(orders[0]) - 1
        self.parts = range(len(orders))

    def copy(self, i, s):
        order = self.orders[i]
        link, path = SENDS[s]
        view = self.view(i, flip(self.me, *[order[k] for k in path]))
        return remote(view, view, self.send_sem.at[self.n * i + s], self.recv_sem.at[self.n * i + s], flip(self.me, order[link]))

    def landed(self, i, s):
        order = self.orders[i]
        link, path = SENDS[s]
        return self.view(i, flip(self.me, order[link], *[order[k] for k in path]))

    def start(self, sends, parts=None):
        for s in sends:
            for i in self.parts if parts is None else parts:
                self.copy(i, s).start()

    def arrived(self, sends, parts=None):
        for s in sends:
            for i in self.parts if parts is None else parts:
                self.copy(i, s).wait_recv()

    def sent(self):
        for i in self.parts:
            for s in range(self.n):
                self.copy(i, s).wait_send()


def _layer(x_ref, gain_ref, freq_ref, wq_ref, wk_ref, wv_ref, wo_ref, y_ref,
           xin, a, wkv, wqs, kv2, kvy, qbuf, qy, wo, seen, cos_s, sin_s, state, sems):
    used = [0]

    def take(n):
        first = used[0]
        used[0] += n
        return sems.at[pl.ds(first, n)]

    local = take(LOCAL)
    wi_s, wi_r, kvg_s, kvg_r, qg_s, qg_r, ax_s, ax_r, am_s, am_r = (take(n) for n in (9, 6, 6, 2, 4) for _ in range(2))
    ky_s, ky_r, qy_s, qy_r, kz_s, kz_r, dup_s, dup_r = (take(n) for n in (6, 6, 12, 24) for _ in range(2))
    wp_s, wp_r, wg_s, wg_r, wd_s, wd_r, out_s, out_r = (take(n) for n in (1, 14, 14, 8) for _ in range(2))
    me = lax.axis_index("sp")
    c, z, y, x = (lax.rem(lax.div(me, w), 2) for w in (C, Z, Y, X))
    mate = flip(me, C)
    own_rows = pl.ds(pl.multiple_of(me * ROWS, 32), ROWS)

    barrier = pltpu.get_barrier_semaphore()
    for mask in range(1, 16):
        pl.semaphore_signal(barrier, inc=1, device_id={"sp": flip(me, *[w for w in (C, Z, Y, X) if mask & w])}, device_id_type=MESH)
    load_x = pltpu.make_async_copy(x_ref, xin, local.at[0])
    load_x.start()
    pl.semaphore_wait(barrier, 15)

    TO = ((), (C,), (X,), (X, C))

    def kv_first(rel, src):
        target = flip(me, *TO[rel])
        cols = pl.ds(pl.multiple_of(lax.div(target, 8) * 512, 512), 512)
        if rel == 0:
            return pltpu.make_async_copy(src.at[:, cols], wkv.at[own_rows], local.at[1])
        return remote(src.at[:, cols], wkv.at[own_rows], wi_s.at[rel - 1], wi_r.at[rel - 1], target)

    def q_first(rel, j):
        target = flip(me, *TO[rel])
        head = 4 * lax.div(target, 8) + 2 * j + lax.rem(target, 2)
        cols = pl.ds(pl.multiple_of(head * HEAD, HEAD), HEAD)
        dst = wqs.at[own_rows, pl.ds(j * HEAD, HEAD)]
        if rel == 0:
            return pltpu.make_async_copy(wq_ref.at[:, cols], dst, local.at[2 + j])
        n = 3 + 2 * (rel - 1) + j
        return remote(wq_ref.at[:, cols], dst, wi_s.at[n], wi_r.at[n], target)

    @pl.when(c == 0)
    def _():
        for rel, src in ((1, wv_ref), (0, wk_ref), (2, wk_ref), (3, wv_ref)):
            kv_first(rel, src).start()

    @pl.when(c == 1)
    def _():
        for rel, src in ((1, wk_ref), (0, wv_ref), (2, wv_ref), (3, wk_ref)):
            kv_first(rel, src).start()

    for rel in (1, 0, 2, 3):
        for j in range(2):
            q_first(rel, j).start()

    def rows_of(buf):
        def view(i, device):
            chip = lax.div(flip(device, X) if i else device, 2)
            return buf.at[pl.ds(pl.multiple_of(chip * (2 * ROWS), 64), 2 * ROWS)]
        return view

    kvg = Gather(rows_of(wkv), ((Y, Z), (Z, Y)), me, kvg_s, kvg_r)
    qg = Gather(rows_of(wqs), ((Y, Z), (Z, Y)), me, qg_s, qg_r)

    def quarter(fx, fc):
        return 2 * lax.div(flip(me, *([X] if fx else [])), 8) + lax.rem(flip(me, *([C] if fc else [])), 2)

    mine = quarter(0, 0)

    def a_view(h):
        return a.at[mine, pl.ds(h * 256, 256)]

    def a_mate(h):
        return remote(a_view(h), a_view(h), am_s.at[h], am_r.at[h], mate)

    def a_x(h):
        return remote(a_view(h), a_view(h), ax_s.at[h], ax_r.at[h], flip(me, X))

    def a_pass(h):
        view = a.at[quarter(1, 0), pl.ds(h * 256, 256)]
        return remote(view, view, am_s.at[2 + h], am_r.at[2 + h], mate)

    gain = gain_ref[...].astype(jnp.float32).reshape(1, D)

    def norm(r, _):
        here = pl.ds(pl.multiple_of(r * 64, 64), 64)
        wide = xin[here, :].astype(jnp.float32)
        scale = lax.rsqrt(jnp.mean(wide * wide, -1, keepdims=True) + 1e-6)
        a[mine, here, :] = (wide * scale * gain).astype(jnp.bfloat16)

    kv_first(0, wk_ref).wait()
    kv_first(1, wk_ref).wait_recv()
    kvg.start((0, 1), (0,))
    load_x.wait()
    for h in range(2):
        lax.fori_loop(4 * h, 4 * h + 4, norm, None)
        a_x(h).start()
        a_mate(h).start()
    kv_first(2, wk_ref).wait_recv()
    kv_first(3, wk_ref).wait_recv()
    kvg.start((0, 1), (1,))
    for j in range(2):
        q_first(0, j).wait()
        q_first(1, j).wait_recv()
    kvg.arrived((0,), (0,))
    kvg.start((2,), (0,))
    kvg.arrived((0,), (1,))
    kvg.start((2,), (1,))
    qg.start((0, 1), (0,))
    for j in range(2):
        q_first(2, j).wait_recv()
        q_first(3, j).wait_recv()
    qg.start((0, 1), (1,))
    wown = pl.ds(pl.multiple_of(me * 128, 128), 128)
    keep_w = pltpu.make_async_copy(wo_ref, wo.at[wown], local.at[4])
    pair_w = remote(wo_ref, wo.at[wown], wp_s.at[0], wp_r.at[0], mate)
    keep_w.start()
    pair_w.start()

    for fx in range(2):
        for fc in range(2):
            n = quarter(fx, fc)
            token = 512 * flip(me, *([X] if fx else []), *([C] if fc else []))

            def angles(r, _):
                here = pl.ds(pl.multiple_of(r * 64, 64), 64)
                place = (token + r * 64 + lax.broadcasted_iota(jnp.int32, (64, HALF), 0)).astype(jnp.float32)
                angle = place * freq_ref[...]
                cos_s[n, here, :] = jnp.cos(angle)
                sin_s[n, here, :] = jnp.sin(angle)

            lax.fori_loop(0, 8, angles, None)

    def turned(w, piece, head, plain, out):
        fx, fc, first, n = PIECES[piece]
        t4 = quarter(fx, fc)
        cols = pl.ds(pl.multiple_of(head * HEAD, HEAD), HEAD)

        def body(r, _):
            here = pl.ds(pl.multiple_of(first + r * 256, 256), 256)
            t = dot(a[t4, here, :], w[:, cols], 1, 0).astype(jnp.bfloat16).astype(jnp.float32)
            cos, sin = cos_s[t4, here, :], sin_s[t4, here, :]
            if plain is not None:
                cos, sin = jnp.where(plain == 1, 1.0, cos), jnp.where(plain == 1, 0.0, sin)
            p, q = t[:, : HALF], t[:, HALF :]
            out(r, (p * cos - q * sin).astype(jnp.bfloat16), (q * cos + p * sin).astype(jnp.bfloat16))

        lax.fori_loop(0, n // 256, body, None)

    def token_rows(piece, *bits):
        fx, fc, first, n = PIECES[piece]
        device = flip(me, *([X] if fx else []), *([C] if fc else []), *bits)
        return pl.ds(pl.multiple_of(device * OWN + first, 256), n)

    def kv_view(piece, *bits):
        return kv2.at[c, token_rows(piece, *bits)]

    def stage(buf, piece):
        fx, fc, first, n = PIECES[piece]
        return buf.at[pl.ds(pl.multiple_of(quarter(fx, fc) * OWN + first, 256), n)]

    def q_view(piece, *bits):
        fx, fc, first, n = PIECES[piece]
        device = flip(me, *([X] if fx else []), *([C] if fc else []), *bits)
        slot = 4 * lax.div(device, 8) + 2 * lax.rem(lax.div(device, 4), 2) + lax.rem(device, 2)
        return qbuf.at[pl.ds(pl.multiple_of(slot * OWN + first, 256), n)]

    def write(view):
        def out(r, left, right):
            view[pl.ds(pl.multiple_of(r * 256, 256), 256), : HALF] = left
            view[pl.ds(pl.multiple_of(r * 256, 256), 256), HALF :] = right
        return out

    def kv_y(piece):
        return remote(stage(kvy, piece), kv_view(piece), ky_s.at[piece], ky_r.at[piece], flip(me, Y))

    def q_y(piece):
        return remote(stage(qy, piece), q_view(piece), qy_s.at[piece], qy_r.at[piece], flip(me, Y))

    def kv_z(n):
        view = kv_view(n % 6, *([Y] if n >= 6 else []))
        return remote(view, view, kz_s.at[n], kz_r.at[n], flip(me, Z))

    def dup(n):
        view = kv_view(n % 6, *([Y] if n % 12 >= 6 else []), *([Z] if n >= 12 else []))
        return remote(view, view, dup_s.at[n], dup_r.at[n], mate)

    def project_kv(piece):
        turned(wkv, piece, 1 - y, c, write(stage(kvy, piece)))
        kv_y(piece).start()
        turned(wkv, piece, y, c, write(kv_view(piece)))
        kv_z(piece).start()
        dup(piece).start()

    def project_q(piece):
        turned(wqs, piece, 1 - y, None, write(stage(qy, piece)))
        q_y(piece).start()
        turned(wqs, piece, y, None, write(q_view(piece)))

    def pass_y(piece):
        kv_y(piece).wait_recv()
        kv_z(6 + piece).start()
        dup(6 + piece).start()

    def pass_z(n):
        kv_z(n).wait_recv()
        dup(12 + n).start()

    columns = pl.ds(pl.multiple_of(c * (D // 2), 128), D // 2)
    wg = Gather(lambda i, device: wo.at[pl.ds(pl.multiple_of(lax.div(device, 2) * 256 + i * 128, 128), 128), columns],
                ((X, Y, Z), (Y, Z, X)), me, wg_s, wg_r)

    def wdup(i, s):
        view = wg.landed(i, s)
        return remote(view, view, wd_s.at[7 * i + s], wd_r.at[7 * i + s], mate)

    def wo_in(i, s, *onward):
        wg.copy(i, s).wait_recv()
        for t in onward:
            wg.copy(i, t).start()
        wdup(i, s).start()

    SUM, TOP, LANES = pl.ds(0, HEAD), pl.ds(HEAD, HALF), pl.ds(HEAD + HALF, HALF)
    state[:, :HEAD] = jnp.zeros((4 * TOK, HEAD), jnp.float32)
    state[:, TOP] = jnp.full((4 * TOK, HALF), NEG, jnp.float32)
    state[:, LANES] = jnp.zeros((4 * TOK, HALF), jnp.float32)
    e = HEAD**-0.5 * LOG2E

    def queries(slot, first, n):
        return pl.ds(pl.multiple_of(slot * TOK + first, STRIP), n)

    def scores(at, keys):
        return dot(qbuf[at, :], kv2[0, keys, :], 1, 1)

    def weigh(at, s):
        tiles = s.shape[1] // HALF
        old = state[at, TOP]
        top = jnp.maximum(old, s.max(axis=1, keepdims=True))
        state[at, TOP] = top
        p = jnp.exp2((s - jnp.tile(top, (1, tiles))) * e)
        keep = jnp.exp2((old - top) * e)
        part = p[:, :HALF]
        for t in range(1, tiles):
            part = part + p[:, t * HALF : (t + 1) * HALF]
        state[at, LANES] = state[at, LANES] * keep + part
        return p.astype(jnp.bfloat16), keep

    def add(at, keys, p, keep):
        state[at, SUM] = state[at, SUM] * jnp.tile(keep, (1, 2)) + dot(p, kv2[1, keys, :], 1, 0)

    def whole(slot, j, first=0, n=TOK, hide=None):
        keys = pl.ds(pl.multiple_of(j * TOK, TOK), TOK)
        ats = [queries(slot, first + k, STRIP) for k in range(0, n, STRIP)]
        s = [scores(at, keys) for at in ats]
        if hide is not None:
            s = [hide(first + k * STRIP, t) for k, t in enumerate(s)]
        w = [weigh(at, t) for at, t in zip(ats, s)]
        for at, t in zip(ats, w):
            add(at, keys, *t)

    def later(first, s):
        row = first + lax.broadcasted_iota(jnp.int32, s.shape, 0)
        return jnp.where(row >= lax.broadcasted_iota(jnp.int32, s.shape, 1), s, HIDDEN)

    def diagonal(slot):
        keys = [pl.ds(pl.multiple_of((2 * slot + z) * TOK, TOK), n) for n in (OWN, TOK)]
        ats = [queries(slot, n, OWN) for n in (0, OWN)]
        s = [scores(at, k) for at, k in zip(ats, keys)]
        s = [later(n * OWN, t) for n, t in enumerate(s)]
        w = [weigh(at, t) for at, t in zip(ats, s)]
        for at, k, t in zip(ats, keys, w):
            add(at, k, *t)

    head = pl.ds(pl.multiple_of((2 * (2 * x + y) + c) * HEAD, HEAD), HEAD)

    def place(i):
        fx, fy = lax.div(3 - i, 2), lax.rem(3 - i, 2)
        return x + fx * (1 - 2 * x), y + fy * (1 - 2 * y)

    def out(i, core):
        x2, y2 = place(i)
        to = c if core == 0 else 1 - c
        src = qbuf.at[pl.ds(pl.multiple_of((2 * x2 + y2) * TOK + to * OWN, OWN), OWN)]
        return src, 8 * x2 + 4 * y2 + 2 * z + to, 2 * i + core

    def out_far(i, core):
        src, device, n = out(i, core)
        return remote(src, seen.at[:, head], out_s.at[n], out_r.at[n], device)

    def out_here():
        src, _, _ = out(3, 0)
        return pltpu.make_async_copy(src, seen.at[:, head], local.at[5])

    def slot_of(i):
        x2, y2 = place(i)
        return 2 * x2 + y2

    def near(i):
        slot = slot_of(i)
        lax.fori_loop(4 * x, 2 * slot + z, lambda j, _: whole(slot, j), None)
        diagonal(slot)

    def scale(slot, first, n):
        def scaled(r, _):
            at = queries(slot, first + r * STRIP, STRIP)
            total = state[at, LANES].sum(axis=1, keepdims=True)
            qbuf[at, :] = (state[at, SUM] * (1 / total)).astype(jnp.bfloat16)

        lax.fori_loop(0, n // STRIP, scaled, None)

    def finish(i):
        scale(slot_of(i), 0, TOK)
        pl.when(i == 3)(lambda: out_here().start())
        pl.when(i < 3)(lambda: out_far(i, 0).start())
        out_far(i, 1).start()

    kvg.arrived((1, 2))
    a_mate(0).wait_recv()
    a_mate(1).wait_recv()
    project_kv(0)
    project_kv(1)
    qg.arrived((0,))
    qg.start((2,))
    a_x(0).wait_recv()
    a_pass(0).start()
    pass_y(0)
    qg.arrived((1, 2))
    project_q(0)
    project_q(1)
    pass_y(1)
    project_kv(2)
    a_pass(0).wait_recv()
    project_kv(3)
    keep_w.wait()
    pair_w.wait_recv()
    wg.copy(1, 0).start()
    wg.copy(1, 1).start()
    project_q(2)
    project_q(3)
    wg.copy(0, 0).start()
    wg.copy(1, 3).start()
    for n in range(12):
        if n % 6 < 2:
            pass_z(n)
    for n in range(24):
        if n % 6 < 2:
            dup(n).wait_recv()
    near(3)
    a_x(1).wait_recv()
    a_pass(1).start()
    project_kv(4)
    a_pass(1).wait_recv()
    project_kv(5)
    pass_y(2)
    pass_y(3)
    project_q(4)
    project_q(5)
    q_y(0).wait_recv()
    q_y(1).wait_recv()
    for n in range(2, 6):
        dup(n).wait_recv()

    def ahead(n, _):
        whole(slot_of(1 + x * (1 + n)), (1 - x) * n + x * (2 * y + z))

    ahead(0, c)
    wo_in(1, 0, 4)
    near(2)
    pass_y(4)
    ahead(1, c)
    pass_y(5)
    wg.copy(1, 2).start()
    wg.copy(0, 1).start()
    wg.copy(0, 3).start()
    wo_in(1, 1, 5)
    wo_in(0, 0, 2, 4)
    for n in (2, 3, 8, 9, 4, 5):
        pass_z(n)

    lax.fori_loop(2, 4 - 2 * x, ahead, None)
    for n in (10, 11):
        pass_z(n)
    for piece in range(2, 6):
        q_y(piece).wait_recv()
    for n in range(6, 24):
        if n % 6 > 1:
            dup(n).wait_recv()

    def poll_a():
        wo_in(1, 2, 6)

    def poll_b():
        wo_in(0, 1, 5)

    def poll_c():
        wo_in(0, 2, 6)

    def far_x():
        slot = slot_of(1)
        lax.fori_loop(4 * (1 - x), 2 * slot + z, lambda j, _: whole(slot, j), None)
        diagonal(slot)
        finish(1)
        poll_a()

        @pl.when(x == 0)
        def _():
            lax.fori_loop(2, 4, lambda n, _: finish(n), None)

    def far_diagonal():
        slot = slot_of(0)
        last = 2 * slot + z

        def half(h, _):
            first = h * OWN
            lax.fori_loop(0, last, lambda j, _: whole(slot, j, first, OWN), None)
            whole(slot, last, first, OWN, later)
            scale(slot, first, OWN)
            pl.when(h == c)(lambda: out_far(0, 0).start())
            pl.when(h != c)(lambda: out_far(0, 1).start())
            pl.when((x == 0) & (h == 0))(poll_b)

        lax.fori_loop(0, 2, half, None)

        @pl.when(x == 0)
        def _():
            poll_c()
            poll_d()

    def poll_d():
        for s in (3, 4):
            for i in range(2):
                wo_in(i, s)

    def rest(i):
        slot = slot_of(i)

        def body(k, _):
            whole(slot, lax.rem(2 * y + z + k, 4))
            if i == 3:
                pl.when(k == 1)(poll_c)
                pl.when(k == 2)(poll_d)

        lax.fori_loop(1, 4, body, None)
        finish(i)
        if i == 2:
            poll_b()

    far_x()

    @pl.when(x == 1)
    def _():
        rest(2)

    far_diagonal()

    @pl.when(x == 1)
    def _():
        rest(3)

    def share(i, n):
        at = pl.ds(pl.multiple_of(slot_of(i) * OWN, OWN), OWN)
        return dot(seen[:, at], wo[at, pl.ds(pl.multiple_of(n * OWN, OWN), OWN)], 1, 0)

    def tile(n):
        return pl.ds(pl.multiple_of(n * OWN, OWN), OWN)

    def came(i):
        for core in range(2):
            if i < 3 or core:
                out_far(i, core).wait_recv()

    def rows_came(*over):
        for i in range(2):
            for s, (link, path) in enumerate(SENDS):
                bits = [wg.orders[i][k] for k in (link, *path)]
                if {X, Y}.intersection(bits) == set(over):
                    wdup(i, s).wait_recv()

    def begin(n, _):
        state[tile(n), :] = share(3, n)

    rows_came()
    out_here().wait()
    came(3)
    lax.fori_loop(0, D // OWN, begin, None)
    for i in range(2):
        wo_in(i, 5)
    rows_came(Y)
    rows_came(X)
    came(2)
    came(1)

    def more(n, _):
        state[tile(n), :] += share(1, n) + share(2, n)

    lax.fori_loop(0, D // OWN, more, None)
    for i in range(2):
        wo_in(i, 6)
    def result(n):
        return pltpu.make_async_copy(xin.at[:, tile(n)], y_ref.at[:, tile(n)], local.at[6 + n])

    rows_came(X, Y)
    came(0)
    for n in range(D // OWN):
        cols = tile(n)
        xin[:, cols] = (xin[:, cols].astype(jnp.float32) + (state[cols, :] + share(0, n))).astype(jnp.bfloat16)
        result(n).start()

    for rel in (1, 2, 3):
        kv_first(rel, wk_ref).wait_send()
        for j in range(2):
            q_first(rel, j).wait_send()
    kvg.sent()
    qg.sent()
    for h in range(2):
        a_mate(h).wait_send()
        a_x(h).wait_send()
        a_pass(h).wait_send()
    for piece in range(6):
        kv_y(piece).wait_send()
        q_y(piece).wait_send()
    for n in range(12):
        kv_z(n).wait_send()
    for n in range(24):
        dup(n).wait_send()
    pair_w.wait_send()
    wg.sent()
    for s in range(7):
        for i in range(2):
            wdup(i, s).wait_send()
    for i in range(4):
        for core in range(2):
            if i < 3 or core:
                out_far(i, core).wait_send()
    for n in range(D // OWN):
        result(n).wait()


def layer(x, gain, freq, wq, wk, wv, wo):
    bf, f32 = jnp.bfloat16, jnp.float32
    hbm, vmem = pl.BlockSpec(memory_space=HBM), pl.BlockSpec(memory_space=pltpu.VMEM)
    buffers = ((OWN, D), (4, OWN, D), (D, OWN), (D, OWN), (2, 8 * TOK, HEAD), (4 * OWN, HEAD), (4 * TOK, HEAD), (4 * OWN, HEAD), (4 * OWN, D),
               (OWN, 4 * OWN))
    return pl.pallas_call(
        _layer,
        in_specs=[hbm, vmem, vmem, hbm, hbm, hbm, hbm],
        out_specs=hbm,
        out_shape=jax.ShapeDtypeStruct((OWN, D), bf),
        scratch_shapes=[
            *[pltpu.VMEM(shape, bf) for shape in buffers],
            pltpu.VMEM((4, OWN, HALF), f32), pltpu.VMEM((4, OWN, HALF), f32), pltpu.VMEM((4 * TOK, 2 * HEAD), f32),
            pltpu.SemaphoreType.DMA((SEMS,)),
        ],
        compiler_params=pltpu.CompilerParams(collective_id=0, has_side_effects=True, vmem_limit_bytes=VMEM),
        cost_estimate=pl.CostEstimate(flops=2**36, transcendentals=2**24, bytes_accessed=2**24),
    )(x, gain, freq, wq, wk, wv, wo)


def _pass(y_ref, out_ref, buf, ins, outs):
    def part(n):
        return pl.ds(n * BLOCK, BLOCK)

    def read(n):
        return pltpu.make_async_copy(y_ref.at[part(n)], buf.at[part(n)], ins.at[n])

    def written(n):
        return pltpu.make_async_copy(buf.at[part(n)], out_ref.at[part(n)], outs.at[n])

    for n in range(OWN // BLOCK):
        read(n).start()
    for n in range(OWN // BLOCK):
        read(n).wait()
        written(n).start()
    for n in range(OWN // BLOCK):
        written(n).wait()


def passed(y):
    hbm, sems = pl.BlockSpec(memory_space=HBM), pltpu.SemaphoreType.DMA((OWN // BLOCK,))
    return pl.pallas_call(_pass, in_specs=[hbm], out_specs=hbm, out_shape=jax.ShapeDtypeStruct((OWN, D), y.dtype),
                          scratch_shapes=[pltpu.VMEM((OWN, D), y.dtype), sems, sems])(y)


def solution(mesh):
    def step(x, gain, wq, wk, wv, wo):
        freq = jnp.asarray((THETA ** (-np.arange(HALF) / HALF)).astype(np.float32).reshape(1, HALF))
        return passed(layer(x, gain, freq, wq, wk, wv, wo))

    tokens, whole = P(("dp", "sp"), None), P("sp", None)
    return jax.shard_map(
        step,
        mesh=mesh,
        in_specs=(tokens, P(None), whole, whole, whole, whole),
        out_specs=tokens,
        check_vma=False,
    )
```
